512 devices in a mesh: dp: 64 (over z, y), tensor: 8 (over x, core).
Axes of the slice: x: 4, y: 8, z: 8, core: 2. Of those that a mesh axis runs over, the one named last changes fastest.
Arguments:
- gradient: bfloat16 [64, 512, 8192], P('dp', 'tensor'), may hold values from -110 to 110
- momentum: bfloat16 [64, 512, 8192], P('dp', 'tensor'), may hold values from -6 to 6
- indices: int32 [64, 8, 128, 32], P('dp', 'tensor'), may hold values from 0 to 4095, all different within a row
Outputs:
- new_momentum: bfloat16 [64, 512, 8192], P('dp', 'tensor')
- update: bfloat16 [512, 8192], P('tensor')
The draws below stay inside these ranges and needn't reach their ends.
Inputs may be any that keep to these rules, and one draw needn't show every extreme that they name: The 32 indices of one span of one replica are distinct; index a * 64 + b names row frequency a and column frequency b.
All inputs are finite; a program needn't handle non-finite values.
Results may differ from the reference program's by a relative error of at most 0.0049.
Values may be sent and summed in bfloat16 or wider, within the bound.
No kernel may reach another device: no remote copies, remote signals or barrier semaphores. Data moves between devices by JAX's collectives and lax.ppermute only.
A program may use at most 64 MiB of HBM per device.

```python
import jax
import jax.numpy as jnp
from jax import lax

D = 8192
BLOCK = 64
TOPK = 32
ROWS = 512
REPLICAS = 64


def draw_gradient(key, part):
    keys = jax.random.split(key, 3)
    own = jnp.clip(jax.random.normal(keys[0], (REPLICAS, ROWS, D), jnp.float32), -4.0, 4.0)
    position = jnp.arange(ROWS, dtype=jnp.float32) / ROWS
    rough_rows = jax.random.uniform(keys[1], (ROWS,), jnp.float32, 0.5, 2.0)
    rough_cols = jax.random.uniform(keys[2], (D,), jnp.float32, 0.5, 2.0)
    ramp = 10.0 ** (position - 0.5) * rough_rows
    return (own * ramp[None, :, None] * rough_cols[None, None, :]).astype(jnp.bfloat16)


def levels(rng, extent, shards, least, largest):
    gain, own = 1.0, jax.random.fold_in(rng, 6)
    for dim, parts in shards:
        heights = jnp.exp(jax.random.uniform(jax.random.fold_in(own, dim), (parts,), jnp.float32, least / len(shards), largest / len(shards)))
        gain = gain * jnp.repeat(heights, extent[dim] // parts).reshape([-1 if axis == dim else 1 for axis in range(len(extent))])
    return gain


def choose_distinct(key, rows, amount, top, lift):
    sequence = jax.random.permutation(jax.random.fold_in(key, 1), amount)
    pull = sequence
    for power in range(3):
        pull = pull * pull // amount
    pull = pull * lift // amount
    lots = jax.random.randint(jax.random.fold_in(key, 2), (rows, amount), 0, 4096) + pull
    sure = jax.random.permutation(jax.random.fold_in(key, 3), rows)[jnp.arange(amount) % rows]
    lots = jnp.where(jnp.arange(rows)[:, None] == sure[None, :], 1 << 14, lots)
    priority = lots * amount + jnp.arange(amount)
    return lax.top_k(priority.astype(jnp.int32), top)[1].astype(jnp.int32)


def noise(rng, extent, width, limit, shards=(), kind=jnp.bfloat16):
    loudness = levels(rng, extent, shards, -0.22, 0.18) if shards else 1.0
    array = jax.random.normal(rng, extent, jnp.float32) * width * loudness
    return jnp.minimum(jnp.maximum(array, -limit), limit).astype(kind)


def setup_inputs(seed: int = 0) -> dict:
    arg_keys = jax.random.split(jax.random.key(seed), 4)
    gradient = draw_gradient(jax.random.fold_in(arg_keys[3], 71), 0)
    momentum = noise(arg_keys[1], (REPLICAS, ROWS, D), 1.0, 6.0, ((0, 64), (1, 8)))
    indices = choose_distinct(arg_keys[2], REPLICAS * (ROWS // BLOCK) * (D // BLOCK), BLOCK * BLOCK, TOPK, 0).reshape((REPLICAS, ROWS // BLOCK, D // BLOCK, TOPK))
    return dict(gradient=gradient, momentum=momentum, indices=indices)


EPSILON = 1e-06
DECAY = 0.999

def dct_basis(block_edge):
    frequency = jnp.arange(block_edge, dtype=jnp.float32)[:, None]
    position = jnp.arange(block_edge, dtype=jnp.float32)[None, :]
    waves = jnp.cos(jnp.pi * (2.0 * position + 1.0) * frequency / (2.0 * block_edge))
    weights = jnp.where(frequency == 0.0, jnp.sqrt(1.0 / block_edge), jnp.sqrt(2.0 / block_edge))
    return waves * weights

def reference(gradient, momentum, indices):
    cosines = dct_basis(BLOCK)
    row_blocks = ROWS // BLOCK
    col_blocks = D // BLOCK
    precise = lax.Precision.HIGHEST
    block_rows = jnp.arange(row_blocks, dtype=jnp.int32)[:, None, None]
    block_cols = jnp.arange(col_blocks, dtype=jnp.int32)[None, :, None]

    def to_spans(slab):
        return slab.reshape(row_blocks, BLOCK, col_blocks, BLOCK).transpose(0, 2, 1, 3)

    def from_spans(blocks):
        return blocks.transpose(0, 2, 1, 3).reshape(ROWS, D)

    def compress(operands):
        grad_slab, moment_slab, chosen = operands
        renewed = DECAY * moment_slab.astype(jnp.float32) + grad_slab.astype(jnp.float32)
        spectrum = jnp.einsum('ka,pqab,lb->pqkl', cosines, to_spans(renewed), cosines, precision=precise)
        flattened = spectrum.reshape(row_blocks, col_blocks, BLOCK * BLOCK)
        picked = jnp.take_along_axis(flattened, chosen, axis=2)
        marker = jnp.zeros_like(flattened).at[block_rows, block_cols, chosen].set(1.0)
        retained = (flattened * marker).reshape(row_blocks, col_blocks, BLOCK, BLOCK)
        restored = jnp.einsum('ka,pqkl,lb->pqab', cosines, retained, cosines, precision=precise)
        return ((renewed - from_spans(restored)).astype(jnp.bfloat16), picked.astype(jnp.bfloat16))
    new_momentum, values = lax.map(compress, (gradient, momentum, indices))

    def absorb(running, operands):
        shipped, chosen = operands
        return (running.at[block_rows, block_cols, chosen].add(shipped.astype(jnp.float32)), None)
    start_sum = jnp.zeros((row_blocks, col_blocks, BLOCK * BLOCK), jnp.float32)
    combined, unused = lax.scan(absorb, start_sum, (values, indices))
    combined = combined.reshape(row_blocks, col_blocks, BLOCK, BLOCK)
    decoded = from_spans(jnp.einsum('ka,pqkl,lb->pqab', cosines, combined, cosines, precision=precise))
    spread = jnp.sqrt(jnp.mean(decoded * decoded) + EPSILON)
    update = (decoded / spread).astype(jnp.bfloat16)
    return (new_momentum, update)
```

```python
import functools

import jax
import jax.numpy as jnp
import numpy as np
from jax import lax
from jax.experimental import pallas as pl
from jax.experimental.pallas import tpu as pltpu
from jax.sharding import Mesh
from jax.sharding import PartitionSpec as P

BLOCK = 64
LANES = 256
QUAD = 4
TENSOR = ("tensor_0", "tensor_1")
DP = ("dp_0", "dp_1")

EPSILON = 1e-06
DECAY = 0.999
F32 = jnp.float32
BF16 = jnp.bfloat16


def dct_basis():
    frequency = np.arange(BLOCK, dtype=np.float64)[:, None]
    position = np.arange(BLOCK, dtype=np.float64)[None, :]
    waves = np.cos(np.pi * (2.0 * position + 1.0) * frequency / (2.0 * BLOCK))
    return (waves * np.where(frequency == 0.0, np.sqrt(1.0 / BLOCK), np.sqrt(2.0 / BLOCK))).astype(np.float32)


def constant_halves(x):
    high = x.astype(BF16)
    return high, (x - high.astype(np.float32)).astype(BF16)


def from_left(cosines):
    high, low = constant_halves(cosines)
    return jnp.asarray(np.concatenate([high, high, low], axis=1))


def from_right(cosines):
    return jnp.asarray(np.stack(constant_halves(np.kron(np.eye(QUAD, dtype=np.float32), cosines))))


def halves(x):
    high = x.astype(BF16)
    return high, (x - high.astype(F32)).astype(BF16)


def dot(a, b):
    return lax.dot_general(a, b, (((1,), (0,)), ((), ())), preferred_element_type=F32)


def dot_t(a, b):
    return lax.dot_general(a, b, (((1,), (1,)), ((), ())), preferred_element_type=F32)


def times_right(tiles, right_ref):
    high, low = halves(tiles)
    return dot(high, right_ref[0]) + dot(low, right_ref[0]) + dot(high, right_ref[1])


def times_left(left_ref, tile):
    high, low = halves(tile)
    return dot(left_ref[...], jnp.concatenate([high, low, high], axis=0))


def spread_rows(index_row, tile_lanes=LANES):
    count = index_row.shape[1]
    per_span = count // QUAD
    span = lax.broadcasted_iota(jnp.int32, (1, count), 1) // per_span
    row = (index_row // BLOCK).astype(F32).astype(BF16)
    col = ((index_row % BLOCK) + span * BLOCK).astype(F32).astype(BF16)
    row_levels = lax.broadcasted_iota(jnp.int32, (BLOCK, count), 0).astype(F32).astype(BF16)
    col_levels = lax.broadcasted_iota(jnp.int32, (tile_lanes, count), 0).astype(F32).astype(BF16)
    return row_levels == row, col_levels == col


def spectra(gradient_ref, momentum_ref, right_ref, left_ref, tiles):
    cuts = [slice(t * LANES, (t + 1) * LANES) for t in range(tiles)]
    renewed = [DECAY * momentum_ref[:, c].astype(F32) + gradient_ref[:, c].astype(F32) for c in cuts]
    half = times_right(jnp.concatenate(renewed, axis=0), right_ref)
    return renewed, [times_left(left_ref, half[t * BLOCK : (t + 1) * BLOCK]) for t in range(tiles)]


def pick_kernel(tiles, peers, gradient_ref, momentum_ref, index_ref, right_ref, left_ref, out_ref, picked_ref):
    step = pl.program_id(0)
    _, spectrum = spectra(gradient_ref, momentum_ref, right_ref, left_ref, tiles)
    rows = []
    for t in range(tiles):
        index_row = index_ref[pl.ds(step * tiles + t, 1), :]
        row_hit, col_hit = spread_rows(index_row)
        by_col = dot(spectrum[t].astype(BF16), jnp.where(col_hit, 1.0, 0.0).astype(BF16))
        rows.append(jnp.sum(jnp.where(row_hit, by_col, 0.0), axis=0, keepdims=True))
    picked_ref[pl.ds(pl.multiple_of(step * tiles, tiles), tiles), :] = jnp.concatenate(rows, axis=0)

    @pl.when(step == pl.num_programs(0) - 1)
    def _():
        index = index_ref[...]
        row = index // BLOCK
        scale = jnp.ones(index.shape, F32)
        for bit in range(6):
            scale = jnp.where((row >> bit) & 1 == 1, scale * float(2 ** (2**bit)), scale)
        coded = (BLOCK + index % BLOCK).astype(F32) * scale
        groups, count = index.shape
        selected = count // QUAD
        spans = groups * QUAD
        group_of = lax.broadcasted_iota(jnp.int32, (groups, spans), 1) // QUAD
        copy_group = jnp.where(lax.broadcasted_iota(jnp.int32, (groups, spans), 0) == group_of, 1.0, 0.0).astype(BF16)
        lane = lax.broadcasted_iota(jnp.int32, (count, spans), 0)
        keep = lane // selected == lax.broadcasted_iota(jnp.int32, (count, spans), 1) % QUAD
        lane_of = lax.broadcasted_iota(jnp.int32, (selected, count), 1) % selected
        gather_lane = jnp.where(lax.broadcasted_iota(jnp.int32, (selected, count), 0) == lane_of, 1.0, 0.0).astype(BF16)
        parts = []
        for table in (picked_ref[...], coded):
            spread = dot(jnp.transpose(table).astype(BF16), copy_group)
            parts.append(dot(gather_lane, jnp.where(keep, spread, 0.0).astype(BF16)))
        payload = jnp.concatenate(parts, axis=0).astype(BF16)
        for peer in range(peers):
            out_ref[peer] = payload


def pick(gradient, momentum, index_rows, right, left, peers, steps=4):
    height, columns = gradient.shape
    width = columns // steps
    tiles = width // LANES
    groups, count = index_rows.shape
    selected, spans = count // QUAD, groups * QUAD
    slab = pl.BlockSpec((height, width), lambda i: (0, i))
    whole = lambda shape: pl.BlockSpec(shape, lambda i: (0,) * len(shape))
    return pl.pallas_call(
        functools.partial(pick_kernel, tiles, peers),
        grid=(steps,),
        in_specs=[slab, slab, whole(index_rows.shape), whole(right.shape), whole(left.shape)],
        out_specs=whole((peers, 2 * selected, spans)),
        out_shape=jax.ShapeDtypeStruct((peers, 2 * selected, spans), BF16),
        scratch_shapes=[pltpu.VMEM((groups, count), F32)],
        name="pick",
    )(gradient, momentum, index_rows, right, left)


def remain_kernel(tiles, gradient_ref, momentum_ref, index_ref, right_ref, left_ref, back_right_ref, back_left_ref, out_ref):
    step = pl.program_id(0)
    renewed, spectrum = spectra(gradient_ref, momentum_ref, right_ref, left_ref, tiles)
    kept = []
    for t in range(tiles):
        index_row = index_ref[pl.ds(step * tiles + t, 1), :]
        row_hit, col_hit = spread_rows(index_row)
        one = lambda hit: jnp.where(hit, 1.0, 0.0).astype(BF16)
        marker = dot_t(one(row_hit), one(col_hit))
        kept.append(spectrum[t] * marker)
    half = times_right(jnp.concatenate(kept, axis=0), back_right_ref)
    for t in range(tiles):
        restored = times_left(back_left_ref, half[t * BLOCK : (t + 1) * BLOCK])
        out_ref[:, t * LANES : (t + 1) * LANES] = (renewed[t] - restored).astype(BF16)


def remain(gradient, momentum, index_rows, right, left, back_right, back_left, steps=4):
    height, columns = gradient.shape
    width = columns // steps
    tiles = width // LANES
    slab = pl.BlockSpec((height, width), lambda i: (0, i))
    whole = lambda shape: pl.BlockSpec(shape, lambda i: (0,) * len(shape))
    return pl.pallas_call(
        functools.partial(remain_kernel, tiles),
        grid=(steps,),
        in_specs=[slab, slab] + [whole(a.shape) for a in (index_rows, right, left, back_right, back_left)],
        out_specs=slab,
        out_shape=jax.ShapeDtypeStruct((height, columns), BF16),
        name="remain",
        cost_estimate=pl.CostEstimate(flops=5_000_000_000, bytes_accessed=6 * height * columns, transcendentals=0),
    )(gradient, momentum, index_rows, right, left, back_right, back_left)


CHUNK = 256
UNROLL = 4


def decode_kernel(in_ref, back_right_ref, back_left_ref, after_ref, decoded_ref, energy_ref, value_ref, row_ref, col_ref, sum_ref):
    sources, double, spans = in_ref.shape
    selected = double // 2
    entries = sources * selected
    per = CHUNK // selected
    for c in range(0, entries, CHUNK):
        s = c // selected
        values = jnp.concatenate([in_ref[s + i, :selected, :] for i in range(per)], axis=0)
        code = jnp.concatenate([in_ref[s + i, selected:, :] for i in range(per)], axis=0)
        row = jnp.zeros(code.shape, BF16)
        for shift in (32, 16, 8, 4, 2, 1):
            above = code >= jnp.asarray(BLOCK * 2.0**shift, BF16)
            code = jnp.where(above, code * jnp.asarray(2.0**-shift, BF16), code)
            row = jnp.where(above, row + jnp.asarray(shift, BF16), row)
        value_ref[:, c : c + CHUNK] = jnp.transpose(values.astype(F32))
        row_ref[:, c : c + CHUNK] = jnp.transpose(row.astype(F32))
        col_ref[:, c : c + CHUNK] = jnp.transpose(code.astype(F32) - float(BLOCK))
    levels = lax.broadcasted_iota(jnp.int32, (BLOCK, CHUNK), 0).astype(F32).astype(BF16)
    zero = jnp.zeros((BLOCK, CHUNK), BF16)
    one = jnp.ones((BLOCK, CHUNK), BF16)

    def combine(span):
        total = None
        for c in range(0, entries, CHUNK):
            part = (pl.ds(span, 1), slice(c, c + CHUNK))
            value, row, col = (ref[part].astype(BF16) for ref in (value_ref, row_ref, col_ref))
            by_row = jnp.where(levels == row, jnp.broadcast_to(value, (BLOCK, CHUNK)), zero)
            by_col = jnp.where(levels == col, one, zero)
            term = dot_t(by_row, by_col)
            total = term if total is None else total + term
        return total

    def body(i, energy):
        for u in range(UNROLL):
            tile = i * UNROLL + u
            parts = [combine(tile * QUAD + k) for k in range(QUAD)]
            for p in parts:
                square = p * p
                for r in range(0, BLOCK, 8):
                    energy = energy + square[r : r + 8]
            sum_ref[pl.ds(pl.multiple_of(tile * BLOCK, BLOCK), BLOCK), :] = jnp.concatenate(parts, axis=1)
        return energy

    tiles = spans // QUAD
    energy = lax.fori_loop(0, tiles // UNROLL, body, jnp.zeros((8, BLOCK), F32))
    energy = jnp.concatenate([energy, jnp.zeros_like(energy)], axis=1)
    for peer in range(energy_ref.shape[0]):
        energy_ref[peer] = energy
    batch = 8
    for first in range(0, tiles, batch):
        half = times_right(sum_ref[first * BLOCK : (first + batch) * BLOCK, :], back_right_ref)
        for t in range(batch):
            tile = times_left(back_left_ref, half[t * BLOCK : (t + 1) * BLOCK])
            decoded_ref[:, (first + t) * LANES : (first + t + 1) * LANES] = tile


def decode(received, back_right, back_left, after, rows):
    sources, double, spans = received.shape
    entries = sources * double // 2
    vmem = pl.BlockSpec(memory_space=pltpu.VMEM)
    return pl.pallas_call(
        decode_kernel,
        in_specs=[vmem] * 3 + [pl.BlockSpec(memory_space=pl.ANY)],
        out_specs=[vmem] * 2,
        out_shape=[
            pltpu.VMEM((BLOCK, spans * BLOCK), F32),
            jax.ShapeDtypeStruct((rows, 8, 128), F32),
        ],
        scratch_shapes=[pltpu.VMEM((spans, entries), F32)] * 3 + [pltpu.VMEM((spans // QUAD * BLOCK, LANES), F32)],
        name="decode",
    )(received, back_right, back_left, after)


def scale_kernel(count, decoded_ref, energy_ref, out_ref):
    total = jnp.sum(energy_ref[...], axis=0)
    total = jnp.sum(jnp.sum(total, axis=0, keepdims=True), axis=1, keepdims=True)
    factor = lax.rsqrt(total * (1.0 / count) + EPSILON)
    out_ref[...] = (decoded_ref[...] * factor).astype(BF16)


def scale(decoded, energies, count):
    vmem = pl.BlockSpec(memory_space=pltpu.VMEM)
    return pl.pallas_call(
        functools.partial(scale_kernel, count),
        in_specs=[vmem] * 2,
        out_specs=vmem,
        out_shape=jax.ShapeDtypeStruct(decoded.shape, BF16),
        name="scale",
    )(decoded, energies)


def in_vmem(x):
    return pltpu.with_memory_space_constraint(x, pltpu.VMEM)


def local(gradient, momentum, indices):
    gradient, momentum = gradient[0], momentum[0]
    height, columns = gradient.shape
    cosines = dct_basis()
    right, left = from_right(cosines.T), from_left(cosines)
    back_right, back_left = from_right(cosines), from_left(cosines.T)
    spans, selected = indices.shape[-2:]
    index_rows = indices.reshape(spans // QUAD, QUAD * selected)
    replicas, rows = lax.axis_size(DP), lax.axis_size(TENSOR)
    outgoing = pick(gradient, momentum, index_rows, right, left, replicas)
    received = lax.all_to_all(outgoing, DP, split_axis=0, concat_axis=0, tiled=True)
    new_momentum = remain(gradient, momentum, index_rows, right, left, back_right, back_left)
    decoded, energy = decode(in_vmem(received), back_right, back_left, new_momentum, rows)
    energies = lax.all_to_all(energy, TENSOR, split_axis=0, concat_axis=0, tiled=True)
    update = scale(in_vmem(decoded), in_vmem(energies), height * columns * rows)
    return (new_momentum[None], update)


def solution(mesh):
    split = Mesh(mesh.devices.reshape(8, 8, 4, 2), ("dp_0", "dp_1", "tensor_0", "tensor_1"))
    placed = (P(DP, TENSOR, None), P(DP, TENSOR, None), P(DP, TENSOR, None, None))
    return jax.shard_map(
        local,
        mesh=split,
        in_specs=placed,
        out_specs=(P(DP, TENSOR, None), P(TENSOR, None)),
        check_vma=False,
    )
```

```python
import functools

import jax
import jax.numpy as jnp
import numpy as np
from jax import lax
from jax.experimental import pallas as pl
from jax.experimental.pallas import tpu as pltpu
from jax.sharding import Mesh
from jax.sharding import PartitionSpec as P

BLOCK = 64
LANES = 256
QUAD = 4
TENSOR = ("tensor_0", "tensor_1")
DP = ("dp_0", "dp_1")

EPSILON = 1e-06
DECAY = 0.999
F32 = jnp.float32
BF16 = jnp.bfloat16


def dct_basis():
    frequency = np.arange(BLOCK, dtype=np.float64)[:, None]
    position = np.arange(BLOCK, dtype=np.float64)[None, :]
    waves = np.cos(np.pi * (2.0 * position + 1.0) * frequency / (2.0 * BLOCK))
    return (waves * np.where(frequency == 0.0, np.sqrt(1.0 / BLOCK), np.sqrt(2.0 / BLOCK))).astype(np.float32)


def constant_halves(x):
    high = x.astype(BF16)
    return high, (x - high.astype(np.float32)).astype(BF16)


def from_left(cosines):
    high, low = constant_halves(cosines)
    return jnp.asarray(np.concatenate([high, high, low], axis=1))


def from_right(cosines):
    return jnp.asarray(np.stack(constant_halves(np.kron(np.eye(QUAD, dtype=np.float32), cosines))))


def halves(x):
    high = x.astype(BF16)
    return high, (x - high.astype(F32)).astype(BF16)


def dot(a, b):
    return lax.dot_general(a, b, (((1,), (0,)), ((), ())), preferred_element_type=F32)


def dot_t(a, b):
    return lax.dot_general(a, b, (((1,), (1,)), ((), ())), preferred_element_type=F32)


def times_right(tiles, right_ref):
    high, low = halves(tiles)
    return dot(high, right_ref[0]) + dot(low, right_ref[0]) + dot(high, right_ref[1])


def times_left(left_ref, tile):
    high, low = halves(tile)
    return dot(left_ref[...], jnp.concatenate([high, low, high], axis=0))


def iota(shape, dim, kind=F32):
    return lax.broadcasted_iota(jnp.int32, shape, dim).astype(kind)


def hot(hit):
    return jnp.where(hit, jnp.ones(hit.shape, BF16), jnp.zeros(hit.shape, BF16))


def one_hot(hit):
    return jnp.where(hit, 1.0, 0.0).astype(BF16)


def col_hits(rows_ref, group, groups):
    col = rows_ref[pl.ds(groups + group, 1), :].astype(BF16)
    return hot(iota((LANES, col.shape[1]), 0).astype(BF16) == col)


def row_levels(rows_ref, group):
    row = rows_ref[pl.ds(group, 1), :]
    return row, iota((BLOCK, row.shape[1]), 0)


def spectra(gradient_ref, momentum_ref, right_ref, left_ref, tiles, first=0):
    cuts = [slice((first + t) * LANES, (first + t + 1) * LANES) for t in range(tiles)]
    renewed = [DECAY * momentum_ref[:, c].astype(F32) + gradient_ref[:, c].astype(F32) for c in cuts]
    half = times_right(jnp.concatenate(renewed, axis=0), right_ref)
    return renewed, [times_left(left_ref, half[t * BLOCK : (t + 1) * BLOCK]) for t in range(tiles)]


def lay_rows(index, rows_ref):
    selected, spans = index.shape
    groups, count = spans // QUAD, selected * QUAD
    copies = one_hot(iota((selected, count), 0, jnp.int32) == iota((selected, count), 1, jnp.int32) % selected)
    keep = iota((spans, count), 0, jnp.int32) % QUAD == iota((spans, count), 1, jnp.int32) // selected
    collect = one_hot(iota((groups, spans), 0, jnp.int32) == iota((groups, spans), 1, jnp.int32) // QUAD)
    span_start = (iota((1, count), 1, jnp.int32) // selected * BLOCK).astype(F32)
    for part, table in enumerate((index // BLOCK, index % BLOCK)):
        turned = jnp.transpose(table.astype(F32)).astype(BF16)
        laid = dot(collect, jnp.where(keep, dot(turned, copies), 0.0).astype(BF16))
        rows_ref[part * groups : (part + 1) * groups, :] = laid + span_start if part else laid


def lay_spans(picked):
    groups, count = picked.shape
    spans, selected = groups * QUAD, count // QUAD
    copies = one_hot(iota((groups, spans), 0, jnp.int32) == iota((groups, spans), 1, jnp.int32) // QUAD)
    keep = iota((count, spans), 0, jnp.int32) // selected == iota((count, spans), 1, jnp.int32) % QUAD
    collect = one_hot(iota((selected, count), 0, jnp.int32) == iota((selected, count), 1, jnp.int32) % selected)
    spread = dot(jnp.transpose(picked).astype(BF16), copies)
    return dot(collect, jnp.where(keep, spread, 0.0).astype(BF16))


def pick_kernel(
    steps, gradient_in, momentum_in, index_in, right_in, left_in, out_ref, rows_ref,
    gradient_ref, momentum_ref, index_ref, right_ref, left_ref, payload_ref, loaded, sent
):
    width = gradient_ref.shape[1] // steps
    tiles = width // LANES
    tables = [
        pltpu.make_async_copy(source, target, loaded.at[2 * steps + k])
        for k, (source, target) in enumerate(((index_in, index_ref), (right_in, right_ref), (left_in, left_ref)))
    ]
    loads = []
    for step in range(steps):
        part = (slice(None), pl.ds(step * width, width))
        loads.append(
            [
                pltpu.make_async_copy(source.at[part], target.at[part], loaded.at[2 * step + k])
                for k, (source, target) in enumerate(((gradient_in, gradient_ref), (momentum_in, momentum_ref)))
            ]
        )
    for group in [tables, *loads]:
        for load in group:
            load.start()
    tables[0].wait()
    index = index_ref[...]
    groups = index.shape[1] // QUAD
    lay_rows(index, rows_ref)
    rows = []
    for load in tables[1:]:
        load.wait()
    for step in range(steps):
        for load in loads[step]:
            load.wait()
        _, spectrum = spectra(gradient_ref, momentum_ref, right_ref, left_ref, tiles, step * tiles)
        for t in range(tiles):
            by_col = dot(spectrum[t].astype(BF16), col_hits(rows_ref, step * tiles + t, groups))
            row, levels = row_levels(rows_ref, step * tiles + t)
            rows.append(jnp.sum(jnp.where(levels == row, by_col, 0.0), axis=0, keepdims=True))
    row = index // BLOCK
    scale = jnp.ones(index.shape, F32)
    for bit in range(6):
        scale = jnp.where((row >> bit) & 1 == 1, scale * float(2 ** (2**bit)), scale)
    coded = (BLOCK + index % BLOCK).astype(F32) * scale
    payload_ref[...] = jnp.concatenate([lay_spans(jnp.concatenate(rows, axis=0)), coded], axis=0).astype(BF16)
    for peer in range(out_ref.shape[0]):
        pltpu.make_async_copy(payload_ref, out_ref.at[peer], sent).start()
    pltpu.make_async_copy(out_ref, out_ref, sent).wait()


VMEM = pl.BlockSpec(memory_space=pltpu.VMEM)
HBM = pl.BlockSpec(memory_space=pltpu.HBM)


def whole(shape):
    return pl.BlockSpec(shape, lambda i: (0,) * len(shape))


def pick(gradient, momentum, index, right, left, peers, steps=2):
    selected, spans = index.shape
    return pl.pallas_call(
        functools.partial(pick_kernel, steps),
        in_specs=[HBM] * 5,
        out_specs=[HBM, VMEM],
        out_shape=[
            pltpu.HBM((peers, 2 * selected, spans), BF16),
            pltpu.VMEM((2 * spans // QUAD, selected * QUAD), F32),
        ],
        scratch_shapes=[
            pltpu.VMEM(gradient.shape, BF16),
            pltpu.VMEM(momentum.shape, BF16),
            pltpu.VMEM(index.shape, jnp.int32),
            pltpu.VMEM(right.shape, BF16),
            pltpu.VMEM(left.shape, BF16),
            pltpu.VMEM((2 * selected, spans), BF16),
            pltpu.SemaphoreType.DMA((2 * steps + 3,)),
            pltpu.SemaphoreType.DMA,
        ],
        name="pick",
    )(gradient, momentum, index, right, left)


def remain_kernel(tiles, gradient_ref, momentum_ref, rows_ref, right_ref, left_ref, back_right_ref, back_left_ref, out_ref):
    step = pl.program_id(0)
    groups = rows_ref.shape[0] // 2
    renewed, spectrum = spectra(gradient_ref, momentum_ref, right_ref, left_ref, tiles)
    kept = []
    for t in range(tiles):
        row, levels = row_levels(rows_ref, step * tiles + t)
        marker = dot_t(hot(levels.astype(BF16) == row.astype(BF16)), col_hits(rows_ref, step * tiles + t, groups))
        kept.append(spectrum[t] * marker)
    half = times_right(jnp.concatenate(kept, axis=0), back_right_ref)
    for t in range(tiles):
        restored = times_left(back_left_ref, half[t * BLOCK : (t + 1) * BLOCK])
        out_ref[:, t * LANES : (t + 1) * LANES] = (renewed[t] - restored).astype(BF16)


def remain(gradient, momentum, rows, right, left, back_right, back_left, steps=4):
    height, columns = gradient.shape
    width = columns // steps
    slab = pl.BlockSpec((height, width), lambda i: (0, i))
    return pl.pallas_call(
        functools.partial(remain_kernel, width // LANES),
        grid=(steps,),
        in_specs=[slab, slab, VMEM] + [whole(a.shape) for a in (right, left, back_right, back_left)],
        out_specs=slab,
        out_shape=jax.ShapeDtypeStruct((height, columns), BF16),
        name="remain",
        cost_estimate=pl.CostEstimate(flops=5_000_000_000, bytes_accessed=6 * height * columns, transcendentals=0),
    )(gradient, momentum, rows, right, left, back_right, back_left)


CHUNK = 256
UNROLL = 4


def combine_kernel(in_ref, after_ref, out_ref, energy_out, value_ref, row_ref, col_ref, sum_ref, energy_ref, stored, shared):
    sources, double, spans = in_ref.shape
    selected = double // 2
    entries = sources * selected
    per = CHUNK // selected
    for c in range(0, entries, CHUNK):
        s = c // selected
        values = jnp.concatenate([in_ref[s + i, :selected, :] for i in range(per)], axis=0)
        code = jnp.concatenate([in_ref[s + i, selected:, :] for i in range(per)], axis=0)
        row = jnp.zeros(code.shape, BF16)
        for shift in (32, 16, 8, 4, 2, 1):
            above = code >= jnp.asarray(BLOCK * 2.0**shift, BF16)
            code = jnp.where(above, code * jnp.asarray(2.0**-shift, BF16), code)
            row = jnp.where(above, row + jnp.asarray(shift, BF16), row)
        value_ref[:, c : c + CHUNK] = jnp.transpose(values.astype(F32))
        row_ref[:, c : c + CHUNK] = jnp.transpose(row.astype(F32))
        col_ref[:, c : c + CHUNK] = jnp.transpose(code.astype(F32) - float(BLOCK))
    levels = lax.broadcasted_iota(jnp.int32, (BLOCK, CHUNK), 0).astype(F32).astype(BF16)
    zero = jnp.zeros((BLOCK, CHUNK), BF16)
    one = jnp.ones((BLOCK, CHUNK), BF16)

    def add_up(span):
        total = None
        for c in range(0, entries, CHUNK):
            part = (pl.ds(span, 1), slice(c, c + CHUNK))
            value, row, col = (ref[part].astype(BF16) for ref in (value_ref, row_ref, col_ref))
            by_row = jnp.where(levels == row, jnp.broadcast_to(value, (BLOCK, CHUNK)), zero)
            by_col = jnp.where(levels == col, one, zero)
            term = dot_t(by_row, by_col)
            total = term if total is None else total + term
        return total

    def body(i, energy):
        for u in range(UNROLL):
            tile = i * UNROLL + u
            parts = [add_up(tile * QUAD + k) for k in range(QUAD)]
            for p in parts:
                square = p * p
                for r in range(0, BLOCK, 8):
                    energy = energy + square[r : r + 8]
            sum_ref[pl.ds(pl.multiple_of(tile * BLOCK, BLOCK), BLOCK), :] = jnp.concatenate(parts, axis=1)
        part = pl.ds(pl.multiple_of(i * (UNROLL * BLOCK), UNROLL * BLOCK), UNROLL * BLOCK)
        pltpu.make_async_copy(sum_ref.at[part], out_ref.at[part], stored).start()
        return energy

    tiles = spans // QUAD
    energy = lax.fori_loop(0, tiles // UNROLL, body, jnp.zeros((8, BLOCK), F32))
    energy = jnp.concatenate([energy, jnp.zeros_like(energy)], axis=1)
    for peer in range(energy_ref.shape[0]):
        energy_ref[peer] = energy
    share = pltpu.make_async_copy(energy_ref, energy_out, shared)
    share.start()
    pltpu.make_async_copy(sum_ref, out_ref, stored).wait()
    share.wait()


def combine(received, after, rows):
    sources, double, spans = received.shape
    entries = sources * double // 2
    return pl.pallas_call(
        combine_kernel,
        in_specs=[VMEM, HBM],
        out_specs=[HBM, HBM],
        out_shape=[pltpu.HBM((spans // QUAD * BLOCK, LANES), F32), pltpu.HBM((rows, 8, 128), F32)],
        scratch_shapes=[pltpu.VMEM((spans, entries), F32)] * 3
        + [pltpu.VMEM((spans // QUAD * BLOCK, LANES), F32), pltpu.VMEM((rows, 8, 128), F32)]
        + [pltpu.SemaphoreType.DMA] * 2,
        name="combine",
    )(received, after)


def decode_kernel(steps, sum_in, right_ref, left_ref, out_ref, sum_ref, loaded):
    height = sum_ref.shape[0] // steps
    loads = []
    for step in range(steps):
        part = pl.ds(step * height, height)
        loads.append(pltpu.make_async_copy(sum_in.at[part], sum_ref.at[part], loaded.at[step]))
    for load in loads:
        load.start()
    for step in range(steps):
        loads[step].wait()
        half = times_right(sum_ref[step * height : (step + 1) * height, :], right_ref)
        for t in range(height // BLOCK):
            lane = (step * (height // BLOCK) + t) * LANES
            out_ref[:, lane : lane + LANES] = times_left(left_ref, half[t * BLOCK : (t + 1) * BLOCK])


def decode(sums, right, left, steps=4):
    tiles = sums.shape[0] // BLOCK
    return pl.pallas_call(
        functools.partial(decode_kernel, steps),
        in_specs=[HBM, VMEM, VMEM],
        out_specs=VMEM,
        out_shape=pltpu.VMEM((BLOCK, tiles * LANES), F32),
        scratch_shapes=[pltpu.VMEM(sums.shape, F32), pltpu.SemaphoreType.DMA((steps,))],
        compiler_params=pltpu.CompilerParams(vmem_limit_bytes=24 * 2**20),
        name="decode",
        cost_estimate=pl.CostEstimate(flops=2_000_000_000, bytes_accessed=8 * sums.size, transcendentals=0),
    )(sums, right, left)


def scale_kernel(steps, count, decoded_ref, energy_ref, out_ref, scaled_ref, stored):
    total = jnp.sum(energy_ref[...], axis=0)
    total = jnp.sum(jnp.sum(total, axis=0, keepdims=True), axis=1, keepdims=True)
    factor = lax.rsqrt(total * (1.0 / count) + EPSILON)
    width = out_ref.shape[1] // steps
    stores = []
    for step in range(steps):
        part = (slice(None), pl.ds(step * width, width))
        scaled_ref[part] = (decoded_ref[part] * factor).astype(BF16)
        stores.append(pltpu.make_async_copy(scaled_ref.at[part], out_ref.at[part], stored.at[step]))
        stores[-1].start()
    for store in stores:
        store.wait()


def scale(decoded, energies, count, steps=4):
    return pl.pallas_call(
        functools.partial(scale_kernel, steps, count),
        in_specs=[VMEM, VMEM],
        out_specs=HBM,
        out_shape=pltpu.HBM(decoded.shape, BF16),
        scratch_shapes=[pltpu.VMEM(decoded.shape, BF16), pltpu.SemaphoreType.DMA((steps,))],
        compiler_params=pltpu.CompilerParams(vmem_limit_bytes=24 * 2**20),
        name="scale",
    )(decoded, energies)


def in_vmem(x):
    return pltpu.with_memory_space_constraint(x, pltpu.VMEM)


def in_hbm(x):
    return pltpu.with_memory_space_constraint(x, pltpu.HBM)


def local(gradient, momentum, indices):
    gradient, momentum = in_hbm(gradient[0]), in_hbm(momentum[0])
    height, columns = gradient.shape
    cosines = dct_basis()
    right, left = from_right(cosines.T), from_left(cosines)
    back_right, back_left = from_right(cosines), from_left(cosines.T)
    index = indices.reshape(indices.shape[-2:]).T
    replicas, rows = lax.axis_size(DP), lax.axis_size(TENSOR)
    outgoing, index_rows = pick(gradient, momentum, in_hbm(index), in_hbm(right), in_hbm(left), replicas)
    received = lax.all_to_all(outgoing, DP, split_axis=0, concat_axis=0, tiled=True)
    new_momentum = remain(gradient, momentum, index_rows, right, left, back_right, back_left)
    sums, energy = combine(in_vmem(received), in_hbm(new_momentum), rows)
    energies = lax.all_to_all(energy, TENSOR, split_axis=0, concat_axis=0, tiled=True)
    decoded = decode(in_hbm(sums), in_vmem(back_right), in_vmem(back_left))
    update = scale(in_vmem(decoded), in_vmem(energies), height * columns * rows)
    return (new_momentum[None], update)


def solution(mesh):
    split = Mesh(mesh.devices.reshape(8, 8, 4, 2), ("dp_0", "dp_1", "tensor_0", "tensor_1"))
    placed = (P(DP, TENSOR, None), P(DP, TENSOR, None), P(DP, TENSOR, None, None))
    return jax.shard_map(
        local,
        mesh=split,
        in_specs=placed,
        out_specs=(P(DP, TENSOR, None), P(TENSOR, None)),
        check_vma=False,
    )
```

```python
import functools

import jax
import jax.numpy as jnp
import numpy as np
from jax import lax
from jax.experimental import pallas as pl
from jax.experimental.pallas import tpu as pltpu
from jax.sharding import Mesh
from jax.sharding import PartitionSpec as P

BLOCK = 64
LANES = 256
QUAD = 4
TENSOR = ("tensor_0", "tensor_1")
DP = ("dp_0", "dp_1")
EVERY = DP + TENSOR

EPSILON = 1e-06
DECAY = 0.999
F32 = jnp.float32
BF16 = jnp.bfloat16


def dct_basis():
    frequency = np.arange(BLOCK, dtype=np.float64)[:, None]
    position = np.arange(BLOCK, dtype=np.float64)[None, :]
    waves = np.cos(np.pi * (2.0 * position + 1.0) * frequency / (2.0 * BLOCK))
    return (waves * np.where(frequency == 0.0, np.sqrt(1.0 / BLOCK), np.sqrt(2.0 / BLOCK))).astype(np.float32)


def constant_halves(x):
    high = x.astype(BF16)
    return high, (x - high.astype(np.float32)).astype(BF16)


def from_left(cosines):
    high, low = constant_halves(cosines)
    return jnp.asarray(np.concatenate([high, high, low], axis=1))


def from_right(cosines):
    return jnp.asarray(np.stack(constant_halves(np.kron(np.eye(QUAD, dtype=np.float32), cosines))))


def halves(x):
    high = x.astype(BF16)
    return high, (x - high.astype(F32)).astype(BF16)


def dot(a, b):
    return lax.dot_general(a, b, (((1,), (0,)), ((), ())), preferred_element_type=F32)


def dot_t(a, b):
    return lax.dot_general(a, b, (((1,), (1,)), ((), ())), preferred_element_type=F32)


def times_right(tiles, right_ref):
    high, low = halves(tiles)
    return dot(high, right_ref[0]) + dot(low, right_ref[0]) + dot(high, right_ref[1])


def times_left(left_ref, tile):
    high, low = halves(tile)
    return dot(left_ref[...], jnp.concatenate([high, low, high], axis=0))


def iota(shape, dim, kind=F32):
    return lax.broadcasted_iota(jnp.int32, shape, dim).astype(kind)


def hot(hit):
    return jnp.where(hit, jnp.ones(hit.shape, BF16), jnp.zeros(hit.shape, BF16))


def one_hot(hit):
    return jnp.where(hit, 1.0, 0.0).astype(BF16)


def col_hits(rows_ref, group, groups):
    col = rows_ref[pl.ds(groups + group, 1), :].astype(BF16)
    return hot(iota((LANES, col.shape[1]), 0).astype(BF16) == col)


def row_levels(rows_ref, group):
    row = rows_ref[pl.ds(group, 1), :]
    return row, iota((BLOCK, row.shape[1]), 0)


def spectra(gradient_ref, momentum_ref, right_ref, left_ref, tiles, first=0):
    cuts = [slice((first + t) * LANES, (first + t + 1) * LANES) for t in range(tiles)]
    renewed = [DECAY * momentum_ref[:, c].astype(F32) + gradient_ref[:, c].astype(F32) for c in cuts]
    half = times_right(jnp.concatenate(renewed, axis=0), right_ref)
    return renewed, [times_left(left_ref, half[t * BLOCK : (t + 1) * BLOCK]) for t in range(tiles)]


def lay_rows(index, rows_ref):
    selected, spans = index.shape
    groups, count = spans // QUAD, selected * QUAD
    copies = one_hot(iota((selected, count), 0, jnp.int32) == iota((selected, count), 1, jnp.int32) % selected)
    keep = iota((spans, count), 0, jnp.int32) % QUAD == iota((spans, count), 1, jnp.int32) // selected
    collect = one_hot(iota((groups, spans), 0, jnp.int32) == iota((groups, spans), 1, jnp.int32) // QUAD)
    span_start = (iota((1, count), 1, jnp.int32) // selected * BLOCK).astype(F32)
    for part, table in enumerate((index // BLOCK, index % BLOCK)):
        turned = jnp.transpose(table.astype(F32)).astype(BF16)
        laid = dot(collect, jnp.where(keep, dot(turned, copies), 0.0).astype(BF16))
        rows_ref[part * groups : (part + 1) * groups, :] = laid + span_start if part else laid


def pick_kernel(
    steps, gradient_in, momentum_in, index_in, right_in, left_in, out_ref, rows_ref,
    gradient_ref, momentum_ref, index_ref, right_ref, left_ref, payload_ref, loaded, sent
):
    width = gradient_ref.shape[1] // steps
    tiles = width // LANES
    tables = [
        pltpu.make_async_copy(source, target, loaded.at[2 * steps + k])
        for k, (source, target) in enumerate(((index_in, index_ref), (right_in, right_ref), (left_in, left_ref)))
    ]
    loads = []
    for step in range(steps):
        part = (slice(None), pl.ds(step * width, width))
        loads.append(
            [
                pltpu.make_async_copy(source.at[part], target.at[part], loaded.at[2 * step + k])
                for k, (source, target) in enumerate(((gradient_in, gradient_ref), (momentum_in, momentum_ref)))
            ]
        )
    for group in [tables, *loads]:
        for load in group:
            load.start()
    tables[0].wait()
    index = index_ref[...]
    groups = index.shape[1] // QUAD
    lay_rows(index, rows_ref)
    rows = []
    for load in tables[1:]:
        load.wait()
    for step in range(steps):
        for load in loads[step]:
            load.wait()
        _, spectrum = spectra(gradient_ref, momentum_ref, right_ref, left_ref, tiles, step * tiles)
        for t in range(tiles):
            by_col = dot(spectrum[t].astype(BF16), col_hits(rows_ref, step * tiles + t, groups))
            row, levels = row_levels(rows_ref, step * tiles + t)
            rows.append(jnp.sum(jnp.where(levels == row, by_col, 0.0), axis=0, keepdims=True))
    row = rows_ref[:groups, :].astype(jnp.int32)
    scale = jnp.ones(row.shape, F32)
    for bit in range(6):
        scale = jnp.where((row >> bit) & 1 == 1, scale * float(2 ** (2**bit)), scale)
    col = rows_ref[groups:, :].astype(jnp.int32) % BLOCK
    coded = (BLOCK + col).astype(F32) * scale
    picked = jnp.concatenate(rows, axis=0)
    shares = payload_ref.shape[0]
    own = groups // shares
    for share in range(shares):
        part = slice(share * own, (share + 1) * own)
        payload_ref[share] = jnp.concatenate([picked[part], coded[part]], axis=0).astype(BF16)
    core = lax.axis_index(TENSOR[1])
    for peer in range(out_ref.shape[0]):
        along_first, along_second = peer // shares, peer % shares
        share = along_second + (along_first - along_second) * core
        pltpu.make_async_copy(payload_ref.at[share], out_ref.at[peer], sent).start()
    pltpu.make_async_copy(out_ref, out_ref, sent).wait()


VMEM = pl.BlockSpec(memory_space=pltpu.VMEM)
HBM = pl.BlockSpec(memory_space=pltpu.HBM)
LIMIT = pltpu.CompilerParams(vmem_limit_bytes=24 * 2**20)


def whole(shape):
    return pl.BlockSpec(shape, lambda i: (0,) * len(shape))


def pick(gradient, momentum, index, right, left, shares, steps=2):
    selected, spans = index.shape
    groups, count = spans // QUAD, selected * QUAD
    share_shape = (2 * groups // shares, count)
    return pl.pallas_call(
        functools.partial(pick_kernel, steps),
        in_specs=[HBM] * 5,
        out_specs=[HBM, VMEM],
        out_shape=[pltpu.HBM((shares * shares, *share_shape), BF16), pltpu.VMEM((2 * groups, count), F32)],
        scratch_shapes=[
            pltpu.VMEM(gradient.shape, BF16),
            pltpu.VMEM(momentum.shape, BF16),
            pltpu.VMEM(index.shape, jnp.int32),
            pltpu.VMEM(right.shape, BF16),
            pltpu.VMEM(left.shape, BF16),
            pltpu.VMEM((shares, *share_shape), BF16),
            pltpu.SemaphoreType.DMA((2 * steps + 3,)),
            pltpu.SemaphoreType.DMA,
        ],
        name="pick",
    )(gradient, momentum, index, right, left)


def remain_kernel(tiles, gradient_ref, momentum_ref, rows_ref, right_ref, left_ref, back_right_ref, back_left_ref, out_ref):
    step = pl.program_id(0)
    groups = rows_ref.shape[0] // 2
    renewed, spectrum = spectra(gradient_ref, momentum_ref, right_ref, left_ref, tiles)
    kept = []
    for t in range(tiles):
        row, levels = row_levels(rows_ref, step * tiles + t)
        marker = dot_t(hot(levels.astype(BF16) == row.astype(BF16)), col_hits(rows_ref, step * tiles + t, groups))
        kept.append(spectrum[t] * marker)
    half = times_right(jnp.concatenate(kept, axis=0), back_right_ref)
    for t in range(tiles):
        restored = times_left(back_left_ref, half[t * BLOCK : (t + 1) * BLOCK])
        out_ref[:, t * LANES : (t + 1) * LANES] = (renewed[t] - restored).astype(BF16)


def remain(gradient, momentum, rows, right, left, back_right, back_left, steps=4):
    height, columns = gradient.shape
    width = columns // steps
    slab = pl.BlockSpec((height, width), lambda i: (0, i))
    return pl.pallas_call(
        functools.partial(remain_kernel, width // LANES),
        grid=(steps,),
        in_specs=[slab, slab, VMEM] + [whole(a.shape) for a in (right, left, back_right, back_left)],
        out_specs=slab,
        out_shape=jax.ShapeDtypeStruct((height, columns), BF16),
        name="remain",
        cost_estimate=pl.CostEstimate(flops=5_000_000_000, bytes_accessed=6 * height * columns, transcendentals=0),
    )(gradient, momentum, rows, right, left, back_right, back_left)


def combine_kernel(in_ref, right_ref, left_ref, block_ref, energy_ref, stage_ref, table_ref, sum_ref):
    sources, double, count = in_ref.shape
    groups, selected = double // 2, count // QUAD
    halved = 128 // sources
    rows = selected // halved
    for source in range(sources):
        stage_ref[source * double : (source + 1) * double, :] = in_ref[source].astype(F32)

    def turned(table):
        shifted = [table] + [pltpu.roll(table, count - h * rows, 1) for h in range(1, halved)]
        return jnp.transpose(jnp.concatenate(shifted, axis=0))

    for g in range(groups):
        value = stage_ref[pl.ds(g, sources, stride=double), :]
        code = stage_ref[pl.ds(groups + g, sources, stride=double), :]
        row = jnp.zeros(code.shape, F32)
        for shift in (32, 16, 8, 4, 2, 1):
            above = code >= BLOCK * 2.0**shift
            code = jnp.where(above, code * 2.0**-shift, code)
            row = jnp.where(above, row + float(shift), row)
        for k, table in enumerate((value, row, code - float(BLOCK))):
            table_ref[3 * g + k] = turned(table)
    levels = iota((BLOCK, 2 * 128), 0).astype(BF16)
    zero = jnp.zeros(levels.shape, BF16)
    one = jnp.ones(levels.shape, BF16)
    energy = jnp.zeros((8, BLOCK), F32)
    for g in range(groups):
        parts = []
        for q in range(QUAD):
            total = None
            for r in range(0, rows, 2):
                at = q * selected + r
                value, row, col = (
                    jnp.concatenate([table_ref[3 * g + k, at + i : at + i + 1, :] for i in range(2)], axis=1).astype(BF16)
                    for k in range(3)
                )
                by_row = jnp.where(levels == row, jnp.broadcast_to(value, levels.shape), zero)
                term = dot_t(by_row, jnp.where(levels == col, one, zero))
                total = term if total is None else total + term
            square = total * total
            for r in range(0, BLOCK, 8):
                energy = energy + square[r : r + 8]
            parts.append(total)
        sum_ref[g * BLOCK : (g + 1) * BLOCK, :] = jnp.concatenate(parts, axis=1)
    energy = jnp.concatenate([energy, jnp.zeros_like(energy)], axis=1)
    for peer in range(energy_ref.shape[0]):
        energy_ref[peer] = energy
    half = times_right(sum_ref[...], right_ref)
    for g in range(groups):
        tile = times_left(left_ref, half[g * BLOCK : (g + 1) * BLOCK]).astype(BF16)
        for k in range(LANES // 128):
            at = (g * (LANES // 128) + k) * BLOCK
            block_ref[at : at + BLOCK, :] = tile[:, k * 128 : (k + 1) * 128]


def combine(received, right, left, rows):
    sources, double, count = received.shape
    height = double // 2 * BLOCK
    return pl.pallas_call(
        combine_kernel,
        in_specs=[VMEM] * 3,
        out_specs=[VMEM, VMEM],
        out_shape=[
            jax.ShapeDtypeStruct((height * LANES // 128, 128), BF16),
            jax.ShapeDtypeStruct((rows, 8, 128), F32),
        ],
        scratch_shapes=[
            pltpu.VMEM((sources * double, count), F32),
            pltpu.VMEM((3 * double // 2, 128, 128), F32),
            pltpu.VMEM((height, LANES), F32),
        ],
        compiler_params=LIMIT,
        name="combine",
    )(received, right, left)


def pack_kernel(block_in, energy_ref, out_ref, block_ref, stamp_ref, loaded, sent):
    height = block_ref.shape[0]
    load = pltpu.make_async_copy(block_in, block_ref, loaded)
    load.start()
    total = jnp.sum(energy_ref[...], axis=0)
    total = jnp.sum(jnp.sum(total, axis=0, keepdims=True), axis=1, keepdims=True)
    pieces = []
    for _ in range(3):
        pieces.append(total.astype(BF16).astype(F32))
        total = total - pieces[-1]
    at = iota(stamp_ref.shape, 0, jnp.int32)
    stamp = jnp.zeros(stamp_ref.shape, F32)
    for k, piece in enumerate(pieces):
        stamp = jnp.where(at == k, piece, stamp)
    stamp_ref[...] = stamp.astype(BF16)
    load.wait()
    for peer in range(out_ref.shape[0]):
        pltpu.make_async_copy(block_ref, out_ref.at[peer, pl.ds(0, height)], sent).start()
        pltpu.make_async_copy(stamp_ref, out_ref.at[peer, pl.ds(height, 8)], sent).start()
    pltpu.make_async_copy(out_ref, out_ref, sent).wait()


def pack(block, energies, peers):
    height, lanes = block.shape
    return pl.pallas_call(
        pack_kernel,
        in_specs=[HBM, VMEM],
        out_specs=HBM,
        out_shape=pltpu.HBM((peers, height + 8, lanes), BF16),
        scratch_shapes=[pltpu.VMEM(block.shape, BF16), pltpu.VMEM((8, lanes), BF16)] + [pltpu.SemaphoreType.DMA] * 2,
        compiler_params=LIMIT,
        name="pack",
    )(block, energies)


def scale_kernel(count, in_ref, after_ref, out_ref, scaled_ref, stored):
    shares, height, lanes = in_ref.shape
    height = height - 8
    total = jnp.zeros((1, 1), F32)
    for share in range(shares):
        stamp = in_ref[share, height:, :].astype(F32)
        total = total + jnp.sum(stamp[:, :1], axis=0, keepdims=True)
    factor = lax.rsqrt(total * (1.0 / count) + EPSILON)
    stores = []
    for share in range(shares):
        pieces = height // BLOCK
        for piece in range(pieces):
            tile = in_ref[share, piece * BLOCK : (piece + 1) * BLOCK, :].astype(F32)
            at = (share * pieces + piece) * lanes
            scaled_ref[:, at : at + lanes] = (tile * factor).astype(BF16)
        if share % 2:
            part = (slice(None), pl.ds((share - 1) * pieces * lanes, 2 * pieces * lanes))
            stores.append(pltpu.make_async_copy(scaled_ref.at[part], out_ref.at[part], stored.at[share // 2]))
            stores[-1].start()
    for store in stores:
        store.wait()


def scale(gathered, after, count):
    shares, height, lanes = gathered.shape
    shape = (BLOCK, shares * (height - 8) // BLOCK * lanes)
    return pl.pallas_call(
        functools.partial(scale_kernel, count),
        in_specs=[VMEM, HBM],
        out_specs=HBM,
        out_shape=pltpu.HBM(shape, BF16),
        scratch_shapes=[pltpu.VMEM(shape, BF16), pltpu.SemaphoreType.DMA((shares // 2,))],
        compiler_params=LIMIT,
        name="scale",
    )(gathered, after)


def places():
    sizes = [lax.axis_size(axis) for axis in EVERY]
    return np.arange(np.prod(sizes)).reshape(sizes)


def gather_lines():
    place = places()
    groups = []
    for chip in range(place.shape[2]):
        groups.extend(place[:, :, chip, 0].tolist())
        groups.extend(place[:, :, chip, 1].T.tolist())
    return groups


def share_holders():
    place = places()
    return [
        [*place[first, second, :, 0].tolist(), *place[second, first, :, 1].tolist()]
        for first in range(place.shape[0])
        for second in range(place.shape[1])
    ]


def exchange(copies, groups):
    return lax.all_to_all(copies, EVERY, split_axis=0, concat_axis=0, axis_index_groups=groups, tiled=True)


def in_vmem(x):
    return pltpu.with_memory_space_constraint(x, pltpu.VMEM)


def in_hbm(x):
    return pltpu.with_memory_space_constraint(x, pltpu.HBM)


def local(gradient, momentum, indices):
    gradient, momentum = in_hbm(gradient[0]), in_hbm(momentum[0])
    height, columns = gradient.shape
    cosines = dct_basis()
    right, left = from_right(cosines.T), from_left(cosines)
    back_right, back_left = from_right(cosines), from_left(cosines.T)
    index = indices.reshape(indices.shape[-2:]).T
    shares, rows = lax.axis_size(DP[0]), lax.axis_size(TENSOR)
    outgoing, index_rows = pick(gradient, momentum, in_hbm(index), in_hbm(right), in_hbm(left), shares)
    received = lax.all_to_all(outgoing, DP, split_axis=0, concat_axis=0, tiled=True)
    block, energy = combine(in_vmem(received), in_vmem(back_right), in_vmem(back_left), rows)
    energies = exchange(energy, share_holders())
    gathered = exchange(pack(in_hbm(block), in_vmem(energies), shares), gather_lines())
    new_momentum = remain(gradient, momentum, index_rows, right, left, back_right, back_left)
    update = scale(in_vmem(gathered), in_hbm(new_momentum), height * columns * rows)
    return (new_momentum[None], update)


def solution(mesh):
    split = Mesh(mesh.devices.reshape(8, 8, 4, 2), ("dp_0", "dp_1", "tensor_0", "tensor_1"))
    placed = (P(DP, TENSOR, None), P(DP, TENSOR, None), P(DP, TENSOR, None, None))
    return jax.shard_map(
        local,
        mesh=split,
        in_specs=placed,
        out_specs=(P(DP, TENSOR, None), P(TENSOR, None)),
        check_vma=False,
    )
```

```python
import functools

import jax
import jax.numpy as jnp
import numpy as np
from jax import lax
from jax.experimental import pallas as pl
from jax.experimental.pallas import tpu as pltpu
from jax.sharding import Mesh
from jax.sharding import PartitionSpec as P

BLOCK = 64
LANES = 256
QUAD = 4
TENSOR = ("tensor_0", "tensor_1")
DP = ("dp_0", "dp_1")
EVERY = DP + TENSOR

EPSILON = 1e-06
DECAY = 0.999
F32 = jnp.float32
BF16 = jnp.bfloat16


def dct_basis():
    frequency = np.arange(BLOCK, dtype=np.float64)[:, None]
    position = np.arange(BLOCK, dtype=np.float64)[None, :]
    waves = np.cos(np.pi * (2.0 * position + 1.0) * frequency / (2.0 * BLOCK))
    return (waves * np.where(frequency == 0.0, np.sqrt(1.0 / BLOCK), np.sqrt(2.0 / BLOCK))).astype(np.float32)


def constant_halves(x):
    high = x.astype(BF16)
    return high, (x - high.astype(np.float32)).astype(BF16)


def from_left(cosines):
    high, low = constant_halves(cosines)
    return jnp.asarray(np.concatenate([high, high, low], axis=1))


def from_right(cosines):
    return jnp.asarray(np.stack(constant_halves(np.kron(np.eye(QUAD, dtype=np.float32), cosines))))


def halves(x):
    high = x.astype(BF16)
    return high, (x - high.astype(F32)).astype(BF16)


def dot(a, b):
    return lax.dot_general(a, b, (((1,), (0,)), ((), ())), preferred_element_type=F32)


def dot_t(a, b):
    return lax.dot_general(a, b, (((1,), (1,)), ((), ())), preferred_element_type=F32)


def times_right(tiles, right_ref):
    high, low = halves(tiles)
    return dot(high, right_ref[0]) + dot(low, right_ref[0]) + dot(high, right_ref[1])


def times_left(left_ref, tile):
    high, low = halves(tile)
    return dot(left_ref[...], jnp.concatenate([high, low, high], axis=0))


def iota(shape, dim, kind=F32):
    return lax.broadcasted_iota(jnp.int32, shape, dim).astype(kind)


def hot(hit):
    return jnp.where(hit, jnp.ones(hit.shape, BF16), jnp.zeros(hit.shape, BF16))


def one_hot(hit):
    return jnp.where(hit, 1.0, 0.0).astype(BF16)


def col_hits(rows_ref, group, groups):
    col = rows_ref[pl.ds(groups + group, 1), :].astype(BF16)
    return hot(iota((LANES, col.shape[1]), 0).astype(BF16) == col)


def row_levels(rows_ref, group):
    row = rows_ref[pl.ds(group, 1), :]
    return row, iota((BLOCK, row.shape[1]), 0)


def spectra(gradient_ref, momentum_ref, right_ref, left_ref, tiles, first=0):
    cuts = [slice((first + t) * LANES, (first + t + 1) * LANES) for t in range(tiles)]
    renewed = [DECAY * momentum_ref[:, c].astype(F32) + gradient_ref[:, c].astype(F32) for c in cuts]
    half = times_right(jnp.concatenate(renewed, axis=0), right_ref)
    return renewed, [times_left(left_ref, half[t * BLOCK : (t + 1) * BLOCK]) for t in range(tiles)]


def lay_rows(index, rows_ref):
    selected, spans = index.shape
    groups, count = spans // QUAD, selected * QUAD
    copies = one_hot(iota((selected, count), 0, jnp.int32) == iota((selected, count), 1, jnp.int32) % selected)
    keep = iota((spans, count), 0, jnp.int32) % QUAD == iota((spans, count), 1, jnp.int32) // selected
    collect = one_hot(iota((groups, spans), 0, jnp.int32) == iota((groups, spans), 1, jnp.int32) // QUAD)
    span_start = (iota((1, count), 1, jnp.int32) // selected * BLOCK).astype(F32)
    for part, table in enumerate((index // BLOCK, index % BLOCK)):
        turned = jnp.transpose(table.astype(F32)).astype(BF16)
        laid = dot(collect, jnp.where(keep, dot(turned, copies), 0.0).astype(BF16))
        rows_ref[part * groups : (part + 1) * groups, :] = laid + span_start if part else laid


def pick_kernel(
    steps, gradient_in, momentum_in, index_in, right_in, left_in, out_ref, rows_ref,
    gradient_ref, momentum_ref, index_ref, right_ref, left_ref, payload_ref, loaded, sent
):
    width = gradient_ref.shape[1] // steps
    tiles = width // LANES
    tables = [
        pltpu.make_async_copy(source, target, loaded.at[2 * steps + k])
        for k, (source, target) in enumerate(((index_in, index_ref), (right_in, right_ref), (left_in, left_ref)))
    ]
    loads = []
    for step in range(steps):
        part = (slice(None), pl.ds(step * width, width))
        loads.append(
            [
                pltpu.make_async_copy(source.at[part], target.at[part], loaded.at[2 * step + k])
                for k, (source, target) in enumerate(((gradient_in, gradient_ref), (momentum_in, momentum_ref)))
            ]
        )
    for group in [tables, *loads]:
        for load in group:
            load.start()
    tables[0].wait()
    index = index_ref[...]
    groups = index.shape[1] // QUAD
    lay_rows(index, rows_ref)
    rows = []
    for load in tables[1:]:
        load.wait()
    for step in range(steps):
        for load in loads[step]:
            load.wait()
        _, spectrum = spectra(gradient_ref, momentum_ref, right_ref, left_ref, tiles, step * tiles)
        for t in range(tiles):
            by_col = dot(spectrum[t].astype(BF16), col_hits(rows_ref, step * tiles + t, groups))
            row, levels = row_levels(rows_ref, step * tiles + t)
            rows.append(jnp.sum(jnp.where(levels == row, by_col, 0.0), axis=0, keepdims=True))
    row = rows_ref[:groups, :].astype(jnp.int32)
    scale = jnp.ones(row.shape, F32)
    for bit in range(6):
        scale = jnp.where((row >> bit) & 1 == 1, scale * float(2 ** (2**bit)), scale)
    col = rows_ref[groups:, :].astype(jnp.int32) % BLOCK
    coded = (BLOCK + col).astype(F32) * scale
    picked = jnp.concatenate(rows, axis=0)
    shares = payload_ref.shape[0]
    own = groups // shares
    for share in range(shares):
        part = slice(share * own, (share + 1) * own)
        payload_ref[share] = jnp.concatenate([picked[part], coded[part]], axis=0).astype(BF16)
    core = lax.axis_index(TENSOR[1])
    for peer in range(out_ref.shape[0]):
        along_first, along_second = peer // shares, peer % shares
        share = along_second + (along_first - along_second) * core
        pltpu.make_async_copy(payload_ref.at[share], out_ref.at[peer], sent).start()
    pltpu.make_async_copy(out_ref, out_ref, sent).wait()


VMEM = pl.BlockSpec(memory_space=pltpu.VMEM)
HBM = pl.BlockSpec(memory_space=pltpu.HBM)
LIMIT = pltpu.CompilerParams(vmem_limit_bytes=24 * 2**20)


def whole(shape):
    return pl.BlockSpec(shape, lambda i: (0,) * len(shape))


def pick(gradient, momentum, index, right, left, shares, steps=2):
    selected, spans = index.shape
    groups, count = spans // QUAD, selected * QUAD
    share_shape = (2 * groups // shares, count)
    return pl.pallas_call(
        functools.partial(pick_kernel, steps),
        in_specs=[HBM] * 5,
        out_specs=[HBM, VMEM],
        out_shape=[pltpu.HBM((shares * shares, *share_shape), BF16), pltpu.VMEM((2 * groups, count), F32)],
        scratch_shapes=[
            pltpu.VMEM(gradient.shape, BF16),
            pltpu.VMEM(momentum.shape, BF16),
            pltpu.VMEM(index.shape, jnp.int32),
            pltpu.VMEM(right.shape, BF16),
            pltpu.VMEM(left.shape, BF16),
            pltpu.VMEM((shares, *share_shape), BF16),
            pltpu.SemaphoreType.DMA((2 * steps + 3,)),
            pltpu.SemaphoreType.DMA,
        ],
        name="pick",
    )(gradient, momentum, index, right, left)


def remain_kernel(tiles, gradient_ref, momentum_ref, rows_ref, right_ref, left_ref, back_right_ref, back_left_ref, out_ref):
    step = pl.program_id(0)
    groups = rows_ref.shape[0] // 2
    renewed, spectrum = spectra(gradient_ref, momentum_ref, right_ref, left_ref, tiles)
    kept = []
    for t in range(tiles):
        row, levels = row_levels(rows_ref, step * tiles + t)
        marker = dot_t(hot(levels.astype(BF16) == row.astype(BF16)), col_hits(rows_ref, step * tiles + t, groups))
        kept.append(spectrum[t] * marker)
    half = times_right(jnp.concatenate(kept, axis=0), back_right_ref)
    for t in range(tiles):
        restored = times_left(back_left_ref, half[t * BLOCK : (t + 1) * BLOCK])
        out_ref[:, t * LANES : (t + 1) * LANES] = (renewed[t] - restored).astype(BF16)


def remain(gradient, momentum, rows, right, left, back_right, back_left, steps=4):
    height, columns = gradient.shape
    width = columns // steps
    slab = pl.BlockSpec((height, width), lambda i: (0, i))
    return pl.pallas_call(
        functools.partial(remain_kernel, width // LANES),
        grid=(steps,),
        in_specs=[slab, slab, VMEM] + [whole(a.shape) for a in (right, left, back_right, back_left)],
        out_specs=slab,
        out_shape=jax.ShapeDtypeStruct((height, columns), BF16),
        name="remain",
        cost_estimate=pl.CostEstimate(flops=5_000_000_000, bytes_accessed=6 * height * columns, transcendentals=0),
    )(gradient, momentum, rows, right, left, back_right, back_left)


def combine_kernel(in_ref, right_ref, left_ref, out_ref, stage_ref, table_ref, sum_ref, block_ref, stamp_ref, sent):
    sources, double, count = in_ref.shape
    groups, selected = double // 2, count // QUAD
    halved = 128 // sources
    rows = selected // halved
    for source in range(sources):
        stage_ref[source * double : (source + 1) * double, :] = in_ref[source].astype(F32)

    def turned(table):
        shifted = [table] + [pltpu.roll(table, count - h * rows, 1) for h in range(1, halved)]
        return jnp.transpose(jnp.concatenate(shifted, axis=0))

    for g in range(groups):
        value = stage_ref[pl.ds(g, sources, stride=double), :]
        code = stage_ref[pl.ds(groups + g, sources, stride=double), :]
        row = jnp.zeros(code.shape, F32)
        for shift in (32, 16, 8, 4, 2, 1):
            above = code >= BLOCK * 2.0**shift
            code = jnp.where(above, code * 2.0**-shift, code)
            row = jnp.where(above, row + float(shift), row)
        for k, table in enumerate((value, row, code - float(BLOCK))):
            table_ref[3 * g + k] = turned(table)
    levels = iota((BLOCK, 2 * 128), 0).astype(BF16)
    zero = jnp.zeros(levels.shape, BF16)
    one = jnp.ones(levels.shape, BF16)
    energy = jnp.zeros((8, BLOCK), F32)
    for g in range(groups):
        parts = []
        for q in range(QUAD):
            total = None
            for r in range(0, rows, 2):
                at = q * selected + r
                value, row, col = (
                    jnp.concatenate([table_ref[3 * g + k, at + i : at + i + 1, :] for i in range(2)], axis=1).astype(BF16)
                    for k in range(3)
                )
                by_row = jnp.where(levels == row, jnp.broadcast_to(value, levels.shape), zero)
                term = dot_t(by_row, jnp.where(levels == col, one, zero))
                total = term if total is None else total + term
            square = total * total
            for r in range(0, BLOCK, 8):
                energy = energy + square[r : r + 8]
            parts.append(total)
        sum_ref[g * BLOCK : (g + 1) * BLOCK, :] = jnp.concatenate(parts, axis=1)
    half = times_right(sum_ref[...], right_ref)
    for g in range(groups):
        tile = times_left(left_ref, half[g * BLOCK : (g + 1) * BLOCK]).astype(BF16)
        for k in range(LANES // 128):
            at = (g * (LANES // 128) + k) * BLOCK
            block_ref[at : at + BLOCK, :] = tile[:, k * 128 : (k + 1) * 128]
    height = block_ref.shape[0]
    for peer in range(out_ref.shape[0]):
        pltpu.make_async_copy(block_ref, out_ref.at[peer, pl.ds(0, height)], sent).start()
    total = jnp.sum(jnp.sum(energy, axis=0, keepdims=True), axis=1, keepdims=True)
    at = iota(stamp_ref.shape, 0, jnp.int32)
    stamp = jnp.zeros(stamp_ref.shape, F32)
    for k in range(3):
        piece = total.astype(BF16).astype(F32)
        stamp = jnp.where(at == k, piece, stamp)
        total = total - piece
    stamp_ref[...] = stamp.astype(BF16)
    for peer in range(out_ref.shape[0]):
        pltpu.make_async_copy(stamp_ref, out_ref.at[peer, pl.ds(height, 8)], sent).start()
    pltpu.make_async_copy(out_ref, out_ref, sent).wait()


def combine(received, right, left, peers):
    sources, double, count = received.shape
    height = double // 2 * BLOCK
    block = (height * LANES // 128, 128)
    return pl.pallas_call(
        combine_kernel,
        in_specs=[VMEM] * 3,
        out_specs=HBM,
        out_shape=pltpu.HBM((peers, block[0] + 8, block[1]), BF16),
        scratch_shapes=[
            pltpu.VMEM((sources * double, count), F32),
            pltpu.VMEM((3 * double // 2, 128, 128), F32),
            pltpu.VMEM((height, LANES), F32),
            pltpu.VMEM(block, BF16),
            pltpu.VMEM((8, 128), BF16),
            pltpu.SemaphoreType.DMA,
        ],
        compiler_params=LIMIT,
        name="combine",
    )(received, right, left)


def total_kernel(in_ref, after_ref, out_ref):
    total = jnp.zeros((1, 1), F32)
    for share in range(in_ref.shape[0]):
        total = total + jnp.sum(in_ref[share, in_ref.shape[1] - 8 :, :].astype(F32)[:, :1], axis=0, keepdims=True)
    tile = out_ref.shape[1:]
    corner = jnp.logical_and(iota(tile, 0, jnp.int32) == 0, iota(tile, 1, jnp.int32) == 0)
    tile = jnp.where(corner, total, 0.0)
    for peer in range(out_ref.shape[0]):
        out_ref[peer] = tile


def row_total(gathered, after, rows):
    return pl.pallas_call(
        total_kernel,
        in_specs=[VMEM, HBM],
        out_specs=VMEM,
        out_shape=pltpu.VMEM((rows, 8, 128), F32),
        compiler_params=LIMIT,
        name="row_total",
    )(gathered, after)


def scale_kernel(count, in_ref, energy_ref, out_ref, scaled_ref, stored):
    shares, height, lanes = in_ref.shape
    height = height - 8
    total = jnp.sum(energy_ref[...], axis=0)
    total = jnp.sum(jnp.sum(total, axis=0, keepdims=True), axis=1, keepdims=True)
    factor = lax.rsqrt(total * (1.0 / count) + EPSILON)
    stores = []
    for share in range(shares):
        pieces = height // BLOCK
        for piece in range(pieces):
            tile = in_ref[share, piece * BLOCK : (piece + 1) * BLOCK, :].astype(F32)
            at = (share * pieces + piece) * lanes
            scaled_ref[:, at : at + lanes] = (tile * factor).astype(BF16)
        if share % 2:
            part = (slice(None), pl.ds((share - 1) * pieces * lanes, 2 * pieces * lanes))
            stores.append(pltpu.make_async_copy(scaled_ref.at[part], out_ref.at[part], stored.at[share // 2]))
            stores[-1].start()
    for store in stores:
        store.wait()


def scale(gathered, energies, count):
    shares, height, lanes = gathered.shape
    shape = (BLOCK, shares * (height - 8) // BLOCK * lanes)
    return pl.pallas_call(
        functools.partial(scale_kernel, count),
        in_specs=[VMEM, VMEM],
        out_specs=HBM,
        out_shape=pltpu.HBM(shape, BF16),
        scratch_shapes=[pltpu.VMEM(shape, BF16), pltpu.SemaphoreType.DMA((shares // 2,))],
        compiler_params=LIMIT,
        name="scale",
    )(gathered, energies)


def places():
    sizes = [lax.axis_size(axis) for axis in EVERY]
    return np.arange(np.prod(sizes)).reshape(sizes)


def gather_lines():
    place = places()
    groups = []
    for chip in range(place.shape[2]):
        groups.extend(place[:, :, chip, 0].tolist())
        groups.extend(place[:, :, chip, 1].T.tolist())
    return groups


def exchange(copies, groups):
    return lax.all_to_all(copies, EVERY, split_axis=0, concat_axis=0, axis_index_groups=groups, tiled=True)


def in_vmem(x):
    return pltpu.with_memory_space_constraint(x, pltpu.VMEM)


def in_hbm(x):
    return pltpu.with_memory_space_constraint(x, pltpu.HBM)


def local(gradient, momentum, indices):
    gradient, momentum = in_hbm(gradient[0]), in_hbm(momentum[0])
    height, columns = gradient.shape
    cosines = dct_basis()
    right, left = from_right(cosines.T), from_left(cosines)
    back_right, back_left = from_right(cosines), from_left(cosines.T)
    index = indices.reshape(indices.shape[-2:]).T
    shares, rows = lax.axis_size(DP[0]), lax.axis_size(TENSOR)
    outgoing, index_rows = pick(gradient, momentum, in_hbm(index), in_hbm(right), in_hbm(left), shares)
    received = lax.all_to_all(outgoing, DP, split_axis=0, concat_axis=0, tiled=True)
    shared = combine(in_vmem(received), in_vmem(back_right), in_vmem(back_left), shares)
    new_momentum = remain(gradient, momentum, index_rows, right, left, back_right, back_left)
    gathered = in_vmem(exchange(shared, gather_lines()))
    energy = row_total(gathered, in_hbm(new_momentum), rows)
    energies = lax.all_to_all(energy, TENSOR, split_axis=0, concat_axis=0, tiled=True)
    update = scale(gathered, in_vmem(energies), height * columns * rows)
    return (new_momentum[None], update)


def solution(mesh):
    split = Mesh(mesh.devices.reshape(8, 8, 4, 2), ("dp_0", "dp_1", "tensor_0", "tensor_1"))
    placed = (P(DP, TENSOR, None), P(DP, TENSOR, None), P(DP, TENSOR, None, None))
    return jax.shard_map(
        local,
        mesh=split,
        in_specs=placed,
        out_specs=(P(DP, TENSOR, None), P(TENSOR, None)),
        check_vma=False,
    )
```

```python
import functools

import jax
import jax.numpy as jnp
import numpy as np
from jax import lax
from jax.experimental import pallas as pl
from jax.experimental.pallas import tpu as pltpu
from jax.sharding import Mesh
from jax.sharding import PartitionSpec as P

BLOCK = 64
LANES = 256
QUAD = 4
SHARES = 2
TENSOR = ("tensor_0", "tensor_1")
DP = ("dp_0", "dp_1")
EVERY = DP + TENSOR

EPSILON = 1e-06
DECAY = 0.999
F32 = jnp.float32
BF16 = jnp.bfloat16


def dct_basis():
    frequency = np.arange(BLOCK, dtype=np.float64)[:, None]
    position = np.arange(BLOCK, dtype=np.float64)[None, :]
    waves = np.cos(np.pi * (2.0 * position + 1.0) * frequency / (2.0 * BLOCK))
    return (waves * np.where(frequency == 0.0, np.sqrt(1.0 / BLOCK), np.sqrt(2.0 / BLOCK))).astype(np.float32)


def constant_halves(x):
    high = x.astype(BF16)
    return high, (x - high.astype(np.float32)).astype(BF16)


def from_left(cosines):
    high, low = constant_halves(cosines)
    return jnp.asarray(np.concatenate([high, high, low], axis=1))


def from_right(cosines):
    return jnp.asarray(np.stack(constant_halves(np.kron(np.eye(QUAD, dtype=np.float32), cosines))))


def halves(x):
    high = x.astype(BF16)
    return high, (x - high.astype(F32)).astype(BF16)


def dot(a, b):
    return lax.dot_general(a, b, (((1,), (0,)), ((), ())), preferred_element_type=F32)


def dot_t(a, b):
    return lax.dot_general(a, b, (((1,), (1,)), ((), ())), preferred_element_type=F32)


def times_right(tiles, right_ref):
    high, low = halves(tiles)
    return dot(high, right_ref[0]) + dot(low, right_ref[0]) + dot(high, right_ref[1])


def times_left(left_ref, tile):
    high, low = halves(tile)
    return dot(left_ref[...], jnp.concatenate([high, low, high], axis=0))


def iota(shape, dim, kind=F32):
    return lax.broadcasted_iota(jnp.int32, shape, dim).astype(kind)


def hot(hit):
    return jnp.where(hit, jnp.ones(hit.shape, BF16), jnp.zeros(hit.shape, BF16))


def one_hot(hit):
    return jnp.where(hit, 1.0, 0.0).astype(BF16)


def col_hits(rows_ref, group, groups):
    col = rows_ref[pl.ds(groups + group, 1), :].astype(BF16)
    return hot(iota((LANES, col.shape[1]), 0).astype(BF16) == col)


def row_levels(rows_ref, group):
    row = rows_ref[pl.ds(group, 1), :]
    return row, iota((BLOCK, row.shape[1]), 0)


def spectra(gradient_ref, momentum_ref, right_ref, left_ref, tiles, first=0):
    cuts = [slice((first + t) * LANES, (first + t + 1) * LANES) for t in range(tiles)]
    renewed = [DECAY * momentum_ref[:, c].astype(F32) + gradient_ref[:, c].astype(F32) for c in cuts]
    half = times_right(jnp.concatenate(renewed, axis=0), right_ref)
    return renewed, [times_left(left_ref, half[t * BLOCK : (t + 1) * BLOCK]) for t in range(tiles)]


def lay_rows(index, rows_ref):
    selected, spans = index.shape
    groups, count = spans // QUAD, selected * QUAD
    copies = one_hot(iota((selected, count), 0, jnp.int32) == iota((selected, count), 1, jnp.int32) % selected)
    keep = iota((spans, count), 0, jnp.int32) % QUAD == iota((spans, count), 1, jnp.int32) // selected
    collect = one_hot(iota((groups, spans), 0, jnp.int32) == iota((groups, spans), 1, jnp.int32) // QUAD)
    span_start = (iota((1, count), 1, jnp.int32) // selected * BLOCK).astype(F32)
    for part, table in enumerate((index // BLOCK, index % BLOCK)):
        turned = jnp.transpose(table.astype(F32)).astype(BF16)
        laid = dot(collect, jnp.where(keep, dot(turned, copies), 0.0).astype(BF16))
        rows_ref[part * groups : (part + 1) * groups, :] = laid + span_start if part else laid


def pick_kernel(
    steps, gradient_in, momentum_in, index_in, right_in, left_in, out_ref, rows_ref,
    gradient_ref, momentum_ref, index_ref, right_ref, left_ref, payload_ref, loaded, sent
):
    starts = np.cumsum([0, *steps])
    tables = [
        pltpu.make_async_copy(source, target, loaded.at[2 * len(steps) + k])
        for k, (source, target) in enumerate(((index_in, index_ref), (right_in, right_ref), (left_in, left_ref)))
    ]
    loads = []
    for step, tiles in enumerate(steps):
        part = (slice(None), pl.ds(int(starts[step]) * LANES, tiles * LANES))
        loads.append(
            [
                pltpu.make_async_copy(source.at[part], target.at[part], loaded.at[2 * step + k])
                for k, (source, target) in enumerate(((gradient_in, gradient_ref), (momentum_in, momentum_ref)))
            ]
        )
    for group in [tables, *loads]:
        for load in group:
            load.start()
    tables[0].wait()
    index = index_ref[...]
    groups = index.shape[1] // QUAD
    lay_rows(index, rows_ref)
    rows = []
    for load in tables[1:]:
        load.wait()
    for step, tiles in enumerate(steps):
        for load in loads[step]:
            load.wait()
        first = int(starts[step])
        _, spectrum = spectra(gradient_ref, momentum_ref, right_ref, left_ref, tiles, first)
        for t in range(tiles):
            by_col = dot(spectrum[t].astype(BF16), col_hits(rows_ref, first + t, groups))
            row, levels = row_levels(rows_ref, first + t)
            rows.append(jnp.sum(jnp.where(levels == row, by_col, 0.0), axis=0, keepdims=True))
    row = rows_ref[:groups, :].astype(jnp.int32)
    scale = jnp.ones(row.shape, F32)
    for bit in range(6):
        scale = jnp.where((row >> bit) & 1 == 1, scale * float(2 ** (2**bit)), scale)
    col = rows_ref[groups:, :].astype(jnp.int32) % BLOCK
    coded = (BLOCK + col).astype(F32) * scale
    picked = jnp.concatenate(rows, axis=0)
    shares = payload_ref.shape[0]
    own = groups // shares
    for share in range(shares):
        part = slice(share * own, (share + 1) * own)
        payload_ref[share] = jnp.concatenate([picked[part], coded[part]], axis=0).astype(BF16)
    core = lax.axis_index(TENSOR[1])
    line = lax.axis_size(DP[1])
    for peer in range(out_ref.shape[0]):
        along_first, along_second = peer // line % shares, peer % line % shares
        share = along_second + (along_first - along_second) * core
        pltpu.make_async_copy(payload_ref.at[share], out_ref.at[peer], sent).start()
    pltpu.make_async_copy(out_ref, out_ref, sent).wait()


VMEM = pl.BlockSpec(memory_space=pltpu.VMEM)
HBM = pl.BlockSpec(memory_space=pltpu.HBM)
LIMIT = pltpu.CompilerParams(vmem_limit_bytes=24 * 2**20)


def whole(shape):
    return pl.BlockSpec(shape, lambda i: (0,) * len(shape))


def pick(gradient, momentum, index, right, left, shares, steps=(8, 24)):
    selected, spans = index.shape
    groups, count = spans // QUAD, selected * QUAD
    share_shape = (2 * groups // shares, count)
    return pl.pallas_call(
        functools.partial(pick_kernel, steps),
        in_specs=[HBM] * 5,
        out_specs=[HBM, VMEM],
        out_shape=[pltpu.HBM((lax.axis_size(DP), *share_shape), BF16), pltpu.VMEM((2 * groups, count), F32)],
        scratch_shapes=[
            pltpu.VMEM(gradient.shape, BF16),
            pltpu.VMEM(momentum.shape, BF16),
            pltpu.VMEM(index.shape, jnp.int32),
            pltpu.VMEM(right.shape, BF16),
            pltpu.VMEM(left.shape, BF16),
            pltpu.VMEM((shares, *share_shape), BF16),
            pltpu.SemaphoreType.DMA((2 * len(steps) + 3,)),
            pltpu.SemaphoreType.DMA,
        ],
        name="pick",
    )(gradient, momentum, index, right, left)


def remain_kernel(tiles, gradient_ref, momentum_ref, rows_ref, right_ref, left_ref, back_right_ref, back_left_ref, out_ref):
    step = pl.program_id(0)
    groups = rows_ref.shape[0] // 2
    renewed, spectrum = spectra(gradient_ref, momentum_ref, right_ref, left_ref, tiles)
    kept = []
    for t in range(tiles):
        row, levels = row_levels(rows_ref, step * tiles + t)
        marker = dot_t(hot(levels.astype(BF16) == row.astype(BF16)), col_hits(rows_ref, step * tiles + t, groups))
        kept.append(spectrum[t] * marker)
    half = times_right(jnp.concatenate(kept, axis=0), back_right_ref)
    for t in range(tiles):
        restored = times_left(back_left_ref, half[t * BLOCK : (t + 1) * BLOCK])
        out_ref[:, t * LANES : (t + 1) * LANES] = (renewed[t] - restored).astype(BF16)


def remain(gradient, momentum, rows, right, left, back_right, back_left, steps=4):
    height, columns = gradient.shape
    width = columns // steps
    slab = pl.BlockSpec((height, width), lambda i: (0, i))
    return pl.pallas_call(
        functools.partial(remain_kernel, width // LANES),
        grid=(steps,),
        in_specs=[slab, slab, VMEM] + [whole(a.shape) for a in (right, left, back_right, back_left)],
        out_specs=slab,
        out_shape=jax.ShapeDtypeStruct((height, columns), BF16),
        name="remain",
        cost_estimate=pl.CostEstimate(flops=5_000_000_000, bytes_accessed=6 * height * columns, transcendentals=0),
    )(gradient, momentum, rows, right, left, back_right, back_left)


def combine_kernel(in_ref, right_ref, left_ref, after_ref, out_ref, stage_ref, table_ref, sum_ref, block_ref, stamp_ref, sent):
    sources, double, count = in_ref.shape
    groups, selected = double // 2, count // QUAD
    halved = 128 // sources
    rows = selected // halved
    for source in range(sources):
        stage_ref[source * double : (source + 1) * double, :] = in_ref[source].astype(F32)

    def turned(table):
        shifted = [table] + [pltpu.roll(table, count - h * rows, 1) for h in range(1, halved)]
        return jnp.transpose(jnp.concatenate(shifted, axis=0))

    for g in range(groups):
        value = stage_ref[pl.ds(g, sources, stride=double), :]
        code = stage_ref[pl.ds(groups + g, sources, stride=double), :]
        row = jnp.zeros(code.shape, F32)
        for shift in (32, 16, 8, 4, 2, 1):
            above = code >= BLOCK * 2.0**shift
            code = jnp.where(above, code * 2.0**-shift, code)
            row = jnp.where(above, row + float(shift), row)
        for k, table in enumerate((value, row, code - float(BLOCK))):
            table_ref[3 * g + k] = turned(table)
    levels = iota((BLOCK, 2 * 128), 0).astype(BF16)
    zero = jnp.zeros(levels.shape, BF16)
    one = jnp.ones(levels.shape, BF16)
    energy = jnp.zeros((8, BLOCK), F32)
    for g in range(groups):
        parts = []
        for q in range(QUAD):
            total = None
            for r in range(0, rows, 2):
                at = q * selected + r
                value, row, col = (
                    jnp.concatenate([table_ref[3 * g + k, at + i : at + i + 1, :] for i in range(2)], axis=1).astype(BF16)
                    for k in range(3)
                )
                by_row = jnp.where(levels == row, jnp.broadcast_to(value, levels.shape), zero)
                term = dot_t(by_row, jnp.where(levels == col, one, zero))
                total = term if total is None else total + term
            square = total * total
            for r in range(0, BLOCK, 8):
                energy = energy + square[r : r + 8]
            parts.append(total)
        sum_ref[g * BLOCK : (g + 1) * BLOCK, :] = jnp.concatenate(parts, axis=1)
    half = times_right(sum_ref[...], right_ref)
    for g in range(groups):
        tile = times_left(left_ref, half[g * BLOCK : (g + 1) * BLOCK]).astype(BF16)
        for k in range(LANES // 128):
            at = (g * (LANES // 128) + k) * BLOCK
            block_ref[at : at + BLOCK, :] = tile[:, k * 128 : (k + 1) * 128]
    height = block_ref.shape[0]
    for peer in range(out_ref.shape[0]):
        pltpu.make_async_copy(block_ref, out_ref.at[peer, pl.ds(0, height)], sent).start()
    total = jnp.sum(jnp.sum(energy, axis=0, keepdims=True), axis=1, keepdims=True)
    at = iota(stamp_ref.shape, 0, jnp.int32)
    stamp = jnp.zeros(stamp_ref.shape, F32)
    for k in range(3):
        piece = total.astype(BF16).astype(F32)
        stamp = jnp.where(at == k, piece, stamp)
        total = total - piece
    stamp_ref[...] = stamp.astype(BF16)
    for peer in range(out_ref.shape[0]):
        pltpu.make_async_copy(stamp_ref, out_ref.at[peer, pl.ds(height, 8)], sent).start()
    pltpu.make_async_copy(out_ref, out_ref, sent).wait()


def combine(received, right, left, after, peers):
    sources, double, count = received.shape
    height = double // 2 * BLOCK
    block = (height * LANES // 128, 128)
    return pl.pallas_call(
        combine_kernel,
        in_specs=[VMEM] * 3 + [HBM],
        out_specs=HBM,
        out_shape=pltpu.HBM((peers, block[0] + 8, block[1]), BF16),
        scratch_shapes=[
            pltpu.VMEM((sources * double, count), F32),
            pltpu.VMEM((3 * double // 2, 128, 128), F32),
            pltpu.VMEM((height, LANES), F32),
            pltpu.VMEM(block, BF16),
            pltpu.VMEM((8, 128), BF16),
            pltpu.SemaphoreType.DMA,
        ],
        compiler_params=LIMIT,
        name="combine",
    )(received, right, left, after)


def total_kernel(in_ref, out_ref):
    total = jnp.zeros((1, 1), F32)
    for share in range(in_ref.shape[0]):
        total = total + jnp.sum(in_ref[share, in_ref.shape[1] - 8 :, :].astype(F32)[:, :1], axis=0, keepdims=True)
    tile = out_ref.shape[1:]
    corner = jnp.logical_and(iota(tile, 0, jnp.int32) == 0, iota(tile, 1, jnp.int32) == 0)
    tile = jnp.where(corner, total, 0.0)
    for peer in range(out_ref.shape[0]):
        out_ref[peer] = tile


def row_total(gathered, rows):
    return pl.pallas_call(
        total_kernel,
        in_specs=[VMEM],
        out_specs=VMEM,
        out_shape=pltpu.VMEM((rows, 8, 128), F32),
        compiler_params=LIMIT,
        name="row_total",
    )(gathered)


def scale_kernel(count, in_ref, energy_ref, out_ref, scaled_ref, stored):
    shares, height, lanes = in_ref.shape
    height = height - 8
    total = jnp.sum(energy_ref[...], axis=0)
    total = jnp.sum(jnp.sum(total, axis=0, keepdims=True), axis=1, keepdims=True)
    factor = lax.rsqrt(total * (1.0 / count) + EPSILON)
    stores = []
    pieces = height // BLOCK
    batch = shares * pieces // stored.shape[0]
    for piece in range(shares * pieces):
        inside = piece % pieces * BLOCK
        tile = in_ref[piece // pieces, inside : inside + BLOCK, :].astype(F32)
        scaled_ref[:, piece * lanes : (piece + 1) * lanes] = (tile * factor).astype(BF16)
        if (piece + 1) % batch == 0:
            part = (slice(None), pl.ds((piece + 1 - batch) * lanes, batch * lanes))
            stores.append(pltpu.make_async_copy(scaled_ref.at[part], out_ref.at[part], stored.at[piece // batch]))
            stores[-1].start()
    for store in stores:
        store.wait()


def scale(gathered, energies, count):
    shares, height, lanes = gathered.shape
    shape = (BLOCK, shares * (height - 8) // BLOCK * lanes)
    return pl.pallas_call(
        functools.partial(scale_kernel, count),
        in_specs=[VMEM, VMEM],
        out_specs=HBM,
        out_shape=pltpu.HBM(shape, BF16),
        scratch_shapes=[pltpu.VMEM(shape, BF16), pltpu.SemaphoreType.DMA((4,))],
        compiler_params=LIMIT,
        name="scale",
    )(gathered, energies)


def places():
    sizes = [lax.axis_size(axis) for axis in EVERY]
    return np.arange(np.prod(sizes)).reshape(sizes)


def share_holders(shares):
    place = places()
    groups = []
    for chip in range(place.shape[2]):
        groups.extend(place[:, :, chip, 0].reshape(-1, shares).tolist())
        groups.extend(place[:, :, chip, 1].T.reshape(-1, shares).tolist())
    return groups


def exchange(copies, groups):
    return lax.all_to_all(copies, EVERY, split_axis=0, concat_axis=0, axis_index_groups=groups, tiled=True)


def in_vmem(x):
    return pltpu.with_memory_space_constraint(x, pltpu.VMEM)


def in_hbm(x):
    return pltpu.with_memory_space_constraint(x, pltpu.HBM)


def local(gradient, momentum, indices):
    gradient, momentum = in_hbm(gradient[0]), in_hbm(momentum[0])
    height, columns = gradient.shape
    cosines = dct_basis()
    right, left = from_right(cosines.T), from_left(cosines)
    back_right, back_left = from_right(cosines), from_left(cosines.T)
    index = indices.reshape(indices.shape[-2:]).T
    rows = lax.axis_size(TENSOR)
    outgoing, index_rows = pick(gradient, momentum, in_hbm(index), in_hbm(right), in_hbm(left), SHARES)
    received = lax.all_to_all(outgoing, DP, split_axis=0, concat_axis=0, tiled=True)
    new_momentum = remain(gradient, momentum, index_rows, right, left, back_right, back_left)
    shared = combine(in_vmem(received), in_vmem(back_right), in_vmem(back_left), in_hbm(new_momentum), SHARES)
    gathered = in_vmem(exchange(shared, share_holders(SHARES)))
    energy = row_total(gathered, rows)
    energies = lax.all_to_all(energy, TENSOR, split_axis=0, concat_axis=0, tiled=True)
    update = scale(gathered, in_vmem(energies), height * columns * rows)
    return (new_momentum[None], update)


def solution(mesh):
    split = Mesh(mesh.devices.reshape(8, 8, 4, 2), ("dp_0", "dp_1", "tensor_0", "tensor_1"))
    placed = (P(DP, TENSOR, None), P(DP, TENSOR, None), P(DP, TENSOR, None, None))
    return jax.shard_map(
        local,
        mesh=split,
        in_specs=placed,
        out_specs=(P(DP, TENSOR, None), P(TENSOR, None)),
        check_vma=False,
    )
```

```python
import functools

import jax
import jax.numpy as jnp
import numpy as np
from jax import lax
from jax.experimental import pallas as pl
from jax.experimental.pallas import tpu as pltpu
from jax.sharding import Mesh
from jax.sharding import PartitionSpec as P

BLOCK = 64
LANES = 256
QUAD = 4
SHARES = 8
TENSOR = ("tensor_0", "tensor_1")
DP = ("dp_0", "dp_1")
EVERY = DP + TENSOR

EPSILON = 1e-06
DECAY = 0.999
F32 = jnp.float32
BF16 = jnp.bfloat16


def dct_basis():
    frequency = np.arange(BLOCK, dtype=np.float64)[:, None]
    position = np.arange(BLOCK, dtype=np.float64)[None, :]
    waves = np.cos(np.pi * (2.0 * position + 1.0) * frequency / (2.0 * BLOCK))
    return (waves * np.where(frequency == 0.0, np.sqrt(1.0 / BLOCK), np.sqrt(2.0 / BLOCK))).astype(np.float32)


def constant_halves(x):
    high = x.astype(BF16)
    return high, (x - high.astype(np.float32)).astype(BF16)


def from_left(cosines):
    high, low = constant_halves(cosines)
    return jnp.asarray(np.concatenate([high, high, low], axis=1))


def from_right(cosines):
    return jnp.asarray(np.stack(constant_halves(np.kron(np.eye(QUAD, dtype=np.float32), cosines))))


def halves(x):
    high = x.astype(BF16)
    return high, (x - high.astype(F32)).astype(BF16)


def dot(a, b):
    return lax.dot_general(a, b, (((1,), (0,)), ((), ())), preferred_element_type=F32)


def dot_t(a, b):
    return lax.dot_general(a, b, (((1,), (1,)), ((), ())), preferred_element_type=F32)


def times_right(tiles, right_ref):
    high, low = halves(tiles)
    return dot(high, right_ref[0]) + dot(low, right_ref[0]) + dot(high, right_ref[1])


def times_left(left_ref, tile):
    high, low = halves(tile)
    return dot(left_ref[...], jnp.concatenate([high, low, high], axis=0))


def iota(shape, dim, kind=F32):
    return lax.broadcasted_iota(jnp.int32, shape, dim).astype(kind)


def hot(hit):
    return jnp.where(hit, jnp.ones(hit.shape, BF16), jnp.zeros(hit.shape, BF16))


def one_hot(hit):
    return jnp.where(hit, 1.0, 0.0).astype(BF16)


def col_hits(rows_ref, group, groups):
    col = rows_ref[pl.ds(groups + group, 1), :].astype(BF16)
    return hot(iota((LANES, col.shape[1]), 0).astype(BF16) == col)


def row_levels(rows_ref, group):
    row = rows_ref[pl.ds(group, 1), :]
    return row, iota((BLOCK, row.shape[1]), 0)


def spectra(gradient_ref, momentum_ref, right_ref, left_ref, tiles, first=0):
    cuts = [slice((first + t) * LANES, (first + t + 1) * LANES) for t in range(tiles)]
    renewed = [DECAY * momentum_ref[:, c].astype(F32) + gradient_ref[:, c].astype(F32) for c in cuts]
    half = times_right(jnp.concatenate(renewed, axis=0), right_ref)
    return renewed, [times_left(left_ref, half[t * BLOCK : (t + 1) * BLOCK]) for t in range(tiles)]


def lay_rows(index, rows_ref):
    selected, spans = index.shape
    groups, count = spans // QUAD, selected * QUAD
    copies = one_hot(iota((selected, count), 0, jnp.int32) == iota((selected, count), 1, jnp.int32) % selected)
    keep = iota((spans, count), 0, jnp.int32) % QUAD == iota((spans, count), 1, jnp.int32) // selected
    collect = one_hot(iota((groups, spans), 0, jnp.int32) == iota((groups, spans), 1, jnp.int32) // QUAD)
    span_start = (iota((1, count), 1, jnp.int32) // selected * BLOCK).astype(F32)
    for part, table in enumerate((index // BLOCK, index % BLOCK)):
        turned = jnp.transpose(table.astype(F32)).astype(BF16)
        laid = dot(collect, jnp.where(keep, dot(turned, copies), 0.0).astype(BF16))
        rows_ref[part * groups : (part + 1) * groups, :] = laid + span_start if part else laid


def pick_kernel(
    steps, gradient_in, momentum_in, index_in, right_in, left_in, out_ref, rows_ref,
    gradient_ref, momentum_ref, index_ref, right_ref, left_ref, payload_ref, loaded, sent
):
    starts = np.cumsum([0, *steps])
    tables = [
        pltpu.make_async_copy(source, target, loaded.at[2 * len(steps) + k])
        for k, (source, target) in enumerate(((index_in, index_ref), (right_in, right_ref), (left_in, left_ref)))
    ]
    loads = []
    for step, tiles in enumerate(steps):
        part = (slice(None), pl.ds(int(starts[step]) * LANES, tiles * LANES))
        loads.append(
            [
                pltpu.make_async_copy(source.at[part], target.at[part], loaded.at[2 * step + k])
                for k, (source, target) in enumerate(((gradient_in, gradient_ref), (momentum_in, momentum_ref)))
            ]
        )
    for group in [tables, *loads]:
        for load in group:
            load.start()
    tables[0].wait()
    index = index_ref[...]
    groups = index.shape[1] // QUAD
    lay_rows(index, rows_ref)
    rows = []
    for load in tables[1:]:
        load.wait()
    for step, tiles in enumerate(steps):
        for load in loads[step]:
            load.wait()
        first = int(starts[step])
        _, spectrum = spectra(gradient_ref, momentum_ref, right_ref, left_ref, tiles, first)
        for t in range(tiles):
            by_col = dot(spectrum[t].astype(BF16), col_hits(rows_ref, first + t, groups))
            row, levels = row_levels(rows_ref, first + t)
            rows.append(jnp.sum(jnp.where(levels == row, by_col, 0.0), axis=0, keepdims=True))
    row = rows_ref[:groups, :].astype(jnp.int32)
    scale = jnp.ones(row.shape, F32)
    for bit in range(6):
        scale = jnp.where((row >> bit) & 1 == 1, scale * float(2 ** (2**bit)), scale)
    col = rows_ref[groups:, :].astype(jnp.int32) % BLOCK
    coded = (BLOCK + col).astype(F32) * scale
    picked = jnp.concatenate(rows, axis=0)
    shares = payload_ref.shape[0]
    own = groups // shares
    for share in range(shares):
        part = slice(share * own, (share + 1) * own)
        payload_ref[share] = jnp.concatenate([picked[part], coded[part]], axis=0).astype(BF16)
    core = lax.axis_index(TENSOR[1])
    line = lax.axis_size(DP[1])
    for peer in range(out_ref.shape[0]):
        along_first, along_second = peer // line % shares, peer % line % shares
        share = along_first + (along_second - along_first) * core
        pltpu.make_async_copy(payload_ref.at[share], out_ref.at[peer], sent).start()
    pltpu.make_async_copy(out_ref, out_ref, sent).wait()


VMEM = pl.BlockSpec(memory_space=pltpu.VMEM)
HBM = pl.BlockSpec(memory_space=pltpu.HBM)
LIMIT = pltpu.CompilerParams(vmem_limit_bytes=24 * 2**20)


def whole(shape):
    return pl.BlockSpec(shape, lambda i: (0,) * len(shape))


def pick(gradient, momentum, index, right, left, shares, steps=(8, 24)):
    selected, spans = index.shape
    groups, count = spans // QUAD, selected * QUAD
    share_shape = (2 * groups // shares, count)
    return pl.pallas_call(
        functools.partial(pick_kernel, steps),
        in_specs=[HBM] * 5,
        out_specs=[HBM, VMEM],
        out_shape=[pltpu.HBM((lax.axis_size(DP), *share_shape), BF16), pltpu.VMEM((2 * groups, count), F32)],
        scratch_shapes=[
            pltpu.VMEM(gradient.shape, BF16),
            pltpu.VMEM(momentum.shape, BF16),
            pltpu.VMEM(index.shape, jnp.int32),
            pltpu.VMEM(right.shape, BF16),
            pltpu.VMEM(left.shape, BF16),
            pltpu.VMEM((shares, *share_shape), BF16),
            pltpu.SemaphoreType.DMA((2 * len(steps) + 3,)),
            pltpu.SemaphoreType.DMA,
        ],
        name="pick",
    )(gradient, momentum, index, right, left)


def remain_kernel(tiles, gradient_ref, momentum_ref, rows_ref, right_ref, left_ref, back_right_ref, back_left_ref, out_ref):
    step = pl.program_id(0)
    groups = rows_ref.shape[0] // 2
    renewed, spectrum = spectra(gradient_ref, momentum_ref, right_ref, left_ref, tiles)
    kept = []
    for t in range(tiles):
        row, levels = row_levels(rows_ref, step * tiles + t)
        marker = dot_t(hot(levels.astype(BF16) == row.astype(BF16)), col_hits(rows_ref, step * tiles + t, groups))
        kept.append(spectrum[t] * marker)
    half = times_right(jnp.concatenate(kept, axis=0), back_right_ref)
    for t in range(tiles):
        restored = times_left(back_left_ref, half[t * BLOCK : (t + 1) * BLOCK])
        out_ref[:, t * LANES : (t + 1) * LANES] = (renewed[t] - restored).astype(BF16)


def remain(gradient, momentum, rows, right, left, back_right, back_left, steps=4):
    height, columns = gradient.shape
    width = columns // steps
    slab = pl.BlockSpec((height, width), lambda i: (0, i))
    return pl.pallas_call(
        functools.partial(remain_kernel, width // LANES),
        grid=(steps,),
        in_specs=[slab, slab, VMEM] + [whole(a.shape) for a in (right, left, back_right, back_left)],
        out_specs=slab,
        out_shape=jax.ShapeDtypeStruct((height, columns), BF16),
        name="remain",
        cost_estimate=pl.CostEstimate(flops=5_000_000_000, bytes_accessed=6 * height * columns, transcendentals=0),
    )(gradient, momentum, rows, right, left, back_right, back_left)


def combine_kernel(in_ref, right_ref, left_ref, out_ref, stage_ref, table_ref, sum_ref, block_ref, stamp_ref, sent):
    sources, double, count = in_ref.shape
    groups, selected = double // 2, count // QUAD
    halved = 128 // sources
    rows = selected // halved
    for source in range(sources):
        stage_ref[source * double : (source + 1) * double, :] = in_ref[source].astype(F32)

    def turned(table):
        shifted = [table] + [pltpu.roll(table, count - h * rows, 1) for h in range(1, halved)]
        return jnp.transpose(jnp.concatenate(shifted, axis=0))

    for g in range(groups):
        value = stage_ref[pl.ds(g, sources, stride=double), :]
        code = stage_ref[pl.ds(groups + g, sources, stride=double), :]
        row = jnp.zeros(code.shape, F32)
        for shift in (32, 16, 8, 4, 2, 1):
            above = code >= BLOCK * 2.0**shift
            code = jnp.where(above, code * 2.0**-shift, code)
            row = jnp.where(above, row + float(shift), row)
        for k, table in enumerate((value, row, code - float(BLOCK))):
            table_ref[3 * g + k] = turned(table)
    levels = iota((BLOCK, 2 * 128), 0).astype(BF16)
    zero = jnp.zeros(levels.shape, BF16)
    one = jnp.ones(levels.shape, BF16)
    energy = jnp.zeros((8, BLOCK), F32)
    for g in range(groups):
        parts = []
        for q in range(QUAD):
            total = None
            for r in range(0, rows, 2):
                at = q * selected + r
                value, row, col = (
                    jnp.concatenate([table_ref[3 * g + k, at + i : at + i + 1, :] for i in range(2)], axis=1).astype(BF16)
                    for k in range(3)
                )
                by_row = jnp.where(levels == row, jnp.broadcast_to(value, levels.shape), zero)
                term = dot_t(by_row, jnp.where(levels == col, one, zero))
                total = term if total is None else total + term
            square = total * total
            for r in range(0, BLOCK, 8):
                energy = energy + square[r : r + 8]
            parts.append(total)
        sum_ref[g * BLOCK : (g + 1) * BLOCK, :] = jnp.concatenate(parts, axis=1)
    half = times_right(sum_ref[...], right_ref)
    for g in range(groups):
        tile = times_left(left_ref, half[g * BLOCK : (g + 1) * BLOCK]).astype(BF16)
        for k in range(LANES // 128):
            at = (g * (LANES // 128) + k) * BLOCK
            block_ref[at : at + BLOCK, :] = tile[:, k * 128 : (k + 1) * 128]
    height = block_ref.shape[0]
    for peer in range(out_ref.shape[0]):
        pltpu.make_async_copy(block_ref, out_ref.at[peer, pl.ds(0, height)], sent).start()
    total = jnp.sum(jnp.sum(energy, axis=0, keepdims=True), axis=1, keepdims=True)
    at = iota(stamp_ref.shape, 0, jnp.int32)
    stamp = jnp.zeros(stamp_ref.shape, F32)
    for k in range(3):
        piece = total.astype(BF16).astype(F32)
        stamp = jnp.where(at == k, piece, stamp)
        total = total - piece
    stamp_ref[...] = stamp.astype(BF16)
    for peer in range(out_ref.shape[0]):
        pltpu.make_async_copy(stamp_ref, out_ref.at[peer, pl.ds(height, 8)], sent).start()
    pltpu.make_async_copy(out_ref, out_ref, sent).wait()


def combine(received, right, left, peers):
    sources, double, count = received.shape
    height = double // 2 * BLOCK
    block = (height * LANES // 128, 128)
    return pl.pallas_call(
        combine_kernel,
        in_specs=[VMEM] * 3,
        out_specs=HBM,
        out_shape=pltpu.HBM((peers, block[0] + 8, block[1]), BF16),
        scratch_shapes=[
            pltpu.VMEM((sources * double, count), F32),
            pltpu.VMEM((3 * double // 2, 128, 128), F32),
            pltpu.VMEM((height, LANES), F32),
            pltpu.VMEM(block, BF16),
            pltpu.VMEM((8, 128), BF16),
            pltpu.SemaphoreType.DMA,
        ],
        compiler_params=LIMIT,
        name="combine",
    )(received, right, left)


def total_kernel(in_ref, after_ref, out_ref):
    total = jnp.zeros((1, 1), F32)
    for share in range(in_ref.shape[0]):
        total = total + jnp.sum(in_ref[share, in_ref.shape[1] - 8 :, :].astype(F32)[:, :1], axis=0, keepdims=True)
    tile = out_ref.shape[1:]
    tile = jnp.where(iota(tile, 1, jnp.int32) == 0, total, 0.0)
    for peer in range(out_ref.shape[0]):
        out_ref[peer] = tile


def row_total(gathered, after, rows):
    return pl.pallas_call(
        total_kernel,
        in_specs=[VMEM, HBM],
        out_specs=VMEM,
        out_shape=pltpu.VMEM((rows, 1, 128), F32),
        compiler_params=LIMIT,
        name="row_total",
    )(gathered, after)


def scale_kernel(count, in_ref, energy_ref, out_ref, scaled_ref, stored):
    shares, height, lanes = in_ref.shape
    height = height - 8
    total = jnp.sum(energy_ref[...], axis=0)
    total = jnp.sum(jnp.sum(total, axis=0, keepdims=True), axis=1, keepdims=True)
    factor = lax.rsqrt(total * (1.0 / count) + EPSILON)
    stores = []
    pieces = height // BLOCK
    batch = shares * pieces // stored.shape[0]
    for piece in range(shares * pieces):
        inside = piece % pieces * BLOCK
        tile = in_ref[piece // pieces, inside : inside + BLOCK, :].astype(F32)
        scaled_ref[:, piece * lanes : (piece + 1) * lanes] = (tile * factor).astype(BF16)
        if (piece + 1) % batch == 0:
            part = (slice(None), pl.ds((piece + 1 - batch) * lanes, batch * lanes))
            stores.append(pltpu.make_async_copy(scaled_ref.at[part], out_ref.at[part], stored.at[piece // batch]))
            stores[-1].start()
    for store in stores:
        store.wait()


def scale(gathered, energies, count):
    shares, height, lanes = gathered.shape
    shape = (BLOCK, shares * (height - 8) // BLOCK * lanes)
    return pl.pallas_call(
        functools.partial(scale_kernel, count),
        in_specs=[VMEM, VMEM],
        out_specs=HBM,
        out_shape=pltpu.HBM(shape, BF16),
        scratch_shapes=[pltpu.VMEM(shape, BF16), pltpu.SemaphoreType.DMA((4,))],
        compiler_params=LIMIT,
        name="scale",
    )(gathered, energies)


def places():
    sizes = [lax.axis_size(axis) for axis in EVERY]
    return np.arange(np.prod(sizes)).reshape(sizes)


def share_holders(shares):
    place = places()
    groups = []
    for chip in range(place.shape[2]):
        groups.extend(place[:, :, chip, 0].T.reshape(-1, shares).tolist())
        groups.extend(place[:, :, chip, 1].reshape(-1, shares).tolist())
    return groups


def exchange(copies, groups):
    return lax.all_to_all(copies, EVERY, split_axis=0, concat_axis=0, axis_index_groups=groups, tiled=True)


def in_vmem(x):
    return pltpu.with_memory_space_constraint(x, pltpu.VMEM)


def in_hbm(x):
    return pltpu.with_memory_space_constraint(x, pltpu.HBM)


def local(gradient, momentum, indices):
    gradient, momentum = in_hbm(gradient[0]), in_hbm(momentum[0])
    height, columns = gradient.shape
    cosines = dct_basis()
    right, left = from_right(cosines.T), from_left(cosines)
    back_right, back_left = from_right(cosines), from_left(cosines.T)
    index = indices.reshape(indices.shape[-2:]).T
    rows = lax.axis_size(TENSOR)
    outgoing, index_rows = pick(gradient, momentum, in_hbm(index), in_hbm(right), in_hbm(left), SHARES)
    received = lax.all_to_all(outgoing, DP, split_axis=0, concat_axis=0, tiled=True)
    shared = combine(in_vmem(received), in_vmem(back_right), in_vmem(back_left), SHARES)
    new_momentum = remain(gradient, momentum, index_rows, right, left, back_right, back_left)
    gathered = in_vmem(exchange(shared, share_holders(SHARES)))
    energy = row_total(gathered, in_hbm(new_momentum), rows)
    energies = lax.all_to_all(energy, TENSOR, split_axis=0, concat_axis=0, tiled=True)
    update = scale(gathered, in_vmem(energies), height * columns * rows)
    return (new_momentum[None], update)


def solution(mesh):
    split = Mesh(mesh.devices.reshape(8, 8, 4, 2), ("dp_0", "dp_1", "tensor_0", "tensor_1"))
    placed = (P(DP, TENSOR, None), P(DP, TENSOR, None), P(DP, TENSOR, None, None))
    return jax.shard_map(
        local,
        mesh=split,
        in_specs=placed,
        out_specs=(P(DP, TENSOR, None), P(TENSOR, None)),
        check_vma=False,
    )
```

```python
import functools

import jax
import jax.numpy as jnp
import numpy as np
from jax import lax
from jax.experimental import pallas as pl
from jax.experimental.pallas import tpu as pltpu
from jax.sharding import Mesh
from jax.sharding import PartitionSpec as P

BLOCK = 64
LANES = 256
QUAD = 4
SHARES = 8
TENSOR = ("tensor_0", "tensor_1")
DP = ("dp_0", "dp_1")
EVERY = DP + TENSOR

EPSILON = 1e-06
DECAY = 0.999
F32 = jnp.float32
BF16 = jnp.bfloat16


def dct_basis():
    frequency = np.arange(BLOCK, dtype=np.float64)[:, None]
    position = np.arange(BLOCK, dtype=np.float64)[None, :]
    waves = np.cos(np.pi * (2.0 * position + 1.0) * frequency / (2.0 * BLOCK))
    return (waves * np.where(frequency == 0.0, np.sqrt(1.0 / BLOCK), np.sqrt(2.0 / BLOCK))).astype(np.float32)


def constant_halves(x):
    high = x.astype(BF16)
    return high, (x - high.astype(np.float32)).astype(BF16)


def from_left(cosines):
    high, low = constant_halves(cosines)
    return jnp.asarray(np.concatenate([high, high, low], axis=1))


def from_right(cosines):
    return jnp.asarray(np.stack(constant_halves(np.kron(np.eye(QUAD, dtype=np.float32), cosines))))


def halves(x):
    high = x.astype(BF16)
    return high, (x - high.astype(F32)).astype(BF16)


def dot(a, b):
    return lax.dot_general(a, b, (((1,), (0,)), ((), ())), preferred_element_type=F32)


def dot_t(a, b):
    return lax.dot_general(a, b, (((1,), (1,)), ((), ())), preferred_element_type=F32)


def times_right(tiles, right_ref):
    high, low = halves(tiles)
    return dot(high, right_ref[0]) + dot(low, right_ref[0]) + dot(high, right_ref[1])


def times_left(left_ref, tile):
    high, low = halves(tile)
    return dot(left_ref[...], jnp.concatenate([high, low, high], axis=0))


def iota(shape, dim, kind=F32):
    return lax.broadcasted_iota(jnp.int32, shape, dim).astype(kind)


def hot(hit):
    return jnp.where(hit, jnp.ones(hit.shape, BF16), jnp.zeros(hit.shape, BF16))


def one_hot(hit):
    return jnp.where(hit, 1.0, 0.0).astype(BF16)


def col_hits(rows_ref, group, groups):
    col = rows_ref[pl.ds(groups + group, 1), :].astype(BF16)
    return hot(iota((LANES, col.shape[1]), 0).astype(BF16) == col)


def row_levels(rows_ref, group):
    row = rows_ref[pl.ds(group, 1), :]
    return row, iota((BLOCK, row.shape[1]), 0)


def spectra(gradient_ref, momentum_ref, right_ref, left_ref, tiles, first=0):
    cuts = [slice((first + t) * LANES, (first + t + 1) * LANES) for t in range(tiles)]
    renewed = [DECAY * momentum_ref[:, c].astype(F32) + gradient_ref[:, c].astype(F32) for c in cuts]
    half = times_right(jnp.concatenate(renewed, axis=0), right_ref)
    return renewed, [times_left(left_ref, half[t * BLOCK : (t + 1) * BLOCK]) for t in range(tiles)]


def lay_rows(index, rows_ref):
    selected, spans = index.shape
    groups, count = spans // QUAD, selected * QUAD
    copies = one_hot(iota((selected, count), 0, jnp.int32) == iota((selected, count), 1, jnp.int32) % selected)
    keep = iota((spans, count), 0, jnp.int32) % QUAD == iota((spans, count), 1, jnp.int32) // selected
    collect = one_hot(iota((groups, spans), 0, jnp.int32) == iota((groups, spans), 1, jnp.int32) // QUAD)
    span_start = (iota((1, count), 1, jnp.int32) // selected * BLOCK).astype(F32)
    for part, table in enumerate((index // BLOCK, index % BLOCK)):
        turned = jnp.transpose(table.astype(F32)).astype(BF16)
        laid = dot(collect, jnp.where(keep, dot(turned, copies), 0.0).astype(BF16))
        rows_ref[part * groups : (part + 1) * groups, :] = laid + span_start if part else laid


def pick_kernel(
    steps, gradient_in, momentum_in, index_in, right_in, left_in, out_ref, rows_ref,
    gradient_ref, momentum_ref, index_ref, right_ref, left_ref, payload_ref, loaded
):
    starts = np.cumsum([0, *steps])
    tables = [
        pltpu.make_async_copy(source, target, loaded.at[2 * len(steps) + k])
        for k, (source, target) in enumerate(((index_in, index_ref), (right_in, right_ref), (left_in, left_ref)))
    ]
    loads = []
    for step, tiles in enumerate(steps):
        part = (slice(None), pl.ds(int(starts[step]) * LANES, tiles * LANES))
        loads.append(
            [
                pltpu.make_async_copy(source.at[part], target.at[part], loaded.at[2 * step + k])
                for k, (source, target) in enumerate(((gradient_in, gradient_ref), (momentum_in, momentum_ref)))
            ]
        )
    for group in [tables, *loads]:
        for load in group:
            load.start()
    tables[0].wait()
    index = index_ref[...]
    groups = index.shape[1] // QUAD
    lay_rows(index, rows_ref)
    rows = []
    for load in tables[1:]:
        load.wait()
    for step, tiles in enumerate(steps):
        for load in loads[step]:
            load.wait()
        first = int(starts[step])
        _, spectrum = spectra(gradient_ref, momentum_ref, right_ref, left_ref, tiles, first)
        for t in range(tiles):
            by_col = dot(spectrum[t].astype(BF16), col_hits(rows_ref, first + t, groups))
            row, levels = row_levels(rows_ref, first + t)
            rows.append(jnp.sum(jnp.where(levels == row, by_col, 0.0), axis=0, keepdims=True))
    row = rows_ref[:groups, :].astype(jnp.int32)
    scale = jnp.ones(row.shape, F32)
    for bit in range(6):
        scale = jnp.where((row >> bit) & 1 == 1, scale * float(2 ** (2**bit)), scale)
    col = rows_ref[groups:, :].astype(jnp.int32) % BLOCK
    coded = (BLOCK + col).astype(F32) * scale
    picked = jnp.concatenate(rows, axis=0)
    shares = payload_ref.shape[0]
    own = groups // shares
    for share in range(shares):
        part = slice(share * own, (share + 1) * own)
        payload_ref[share] = jnp.concatenate([picked[part], coded[part]], axis=0).astype(BF16)
    core = lax.axis_index(TENSOR[1])
    line = lax.axis_size(DP[1])
    for peer in range(out_ref.shape[0]):
        along_first, along_second = peer // line % shares, peer % line % shares
        out_ref[peer] = payload_ref[along_first + (along_second - along_first) * core]


VMEM = pl.BlockSpec(memory_space=pltpu.VMEM)
HBM = pl.BlockSpec(memory_space=pltpu.HBM)
LIMIT = pltpu.CompilerParams(vmem_limit_bytes=24 * 2**20)


def whole(shape):
    return pl.BlockSpec(shape, lambda i: (0,) * len(shape))


def pick(gradient, momentum, index, right, left, shares, steps=(8, 24)):
    selected, spans = index.shape
    groups, count = spans // QUAD, selected * QUAD
    share_shape = (2 * groups // shares, count)
    return pl.pallas_call(
        functools.partial(pick_kernel, steps),
        in_specs=[HBM] * 5,
        out_specs=[VMEM, VMEM],
        out_shape=[pltpu.VMEM((lax.axis_size(DP), *share_shape), BF16), pltpu.VMEM((2 * groups, count), F32)],
        scratch_shapes=[
            pltpu.VMEM(gradient.shape, BF16),
            pltpu.VMEM(momentum.shape, BF16),
            pltpu.VMEM(index.shape, jnp.int32),
            pltpu.VMEM(right.shape, BF16),
            pltpu.VMEM(left.shape, BF16),
            pltpu.VMEM((shares, *share_shape), BF16),
            pltpu.SemaphoreType.DMA((2 * len(steps) + 3,)),
        ],
        name="pick",
    )(gradient, momentum, index, right, left)


def remain_kernel(tiles, gradient_ref, momentum_ref, rows_ref, right_ref, left_ref, back_right_ref, back_left_ref, out_ref):
    step = pl.program_id(0)
    groups = rows_ref.shape[0] // 2
    renewed, spectrum = spectra(gradient_ref, momentum_ref, right_ref, left_ref, tiles)
    kept = []
    for t in range(tiles):
        row, levels = row_levels(rows_ref, step * tiles + t)
        marker = dot_t(hot(levels.astype(BF16) == row.astype(BF16)), col_hits(rows_ref, step * tiles + t, groups))
        kept.append(spectrum[t] * marker)
    half = times_right(jnp.concatenate(kept, axis=0), back_right_ref)
    for t in range(tiles):
        restored = times_left(back_left_ref, half[t * BLOCK : (t + 1) * BLOCK])
        out_ref[:, t * LANES : (t + 1) * LANES] = (renewed[t] - restored).astype(BF16)


def remain(gradient, momentum, rows, right, left, back_right, back_left, steps=4):
    height, columns = gradient.shape
    width = columns // steps
    slab = pl.BlockSpec((height, width), lambda i: (0, i))
    return pl.pallas_call(
        functools.partial(remain_kernel, width // LANES),
        grid=(steps,),
        in_specs=[slab, slab, VMEM] + [whole(a.shape) for a in (right, left, back_right, back_left)],
        out_specs=slab,
        out_shape=jax.ShapeDtypeStruct((height, columns), BF16),
        name="remain",
        cost_estimate=pl.CostEstimate(flops=5_000_000_000, bytes_accessed=6 * height * columns, transcendentals=0),
    )(gradient, momentum, rows, right, left, back_right, back_left)


def combine_kernel(in_ref, right_ref, left_ref, out_ref, stage_ref, table_ref, sum_ref, block_ref, stamp_ref, sent):
    sources, double, count = in_ref.shape
    groups, selected = double // 2, count // QUAD
    halved = 128 // sources
    rows = selected // halved
    for source in range(sources):
        stage_ref[source * double : (source + 1) * double, :] = in_ref[source].astype(F32)

    def turned(table):
        shifted = [table] + [pltpu.roll(table, count - h * rows, 1) for h in range(1, halved)]
        return jnp.transpose(jnp.concatenate(shifted, axis=0))

    for g in range(groups):
        value = stage_ref[pl.ds(g, sources, stride=double), :]
        code = stage_ref[pl.ds(groups + g, sources, stride=double), :]
        row = jnp.zeros(code.shape, F32)
        for shift in (32, 16, 8, 4, 2, 1):
            above = code >= BLOCK * 2.0**shift
            code = jnp.where(above, code * 2.0**-shift, code)
            row = jnp.where(above, row + float(shift), row)
        for k, table in enumerate((value, row, code - float(BLOCK))):
            table_ref[3 * g + k] = turned(table)
    levels = iota((BLOCK, 2 * 128), 0).astype(BF16)
    zero = jnp.zeros(levels.shape, BF16)
    one = jnp.ones(levels.shape, BF16)
    energy = jnp.zeros((8, BLOCK), F32)
    for g in range(groups):
        parts = []
        for q in range(QUAD):
            total = None
            for r in range(0, rows, 2):
                at = q * selected + r
                value, row, col = (
                    jnp.concatenate([table_ref[3 * g + k, at + i : at + i + 1, :] for i in range(2)], axis=1).astype(BF16)
                    for k in range(3)
                )
                by_row = jnp.where(levels == row, jnp.broadcast_to(value, levels.shape), zero)
                term = dot_t(by_row, jnp.where(levels == col, one, zero))
                total = term if total is None else total + term
            square = total * total
            for r in range(0, BLOCK, 8):
                energy = energy + square[r : r + 8]
            parts.append(total)
        sum_ref[g * BLOCK : (g + 1) * BLOCK, :] = jnp.concatenate(parts, axis=1)
    height = BLOCK * (LANES // 128)
    batch = groups // 2
    for first in range(0, groups, batch):
        half = times_right(sum_ref[first * BLOCK : (first + batch) * BLOCK, :], right_ref)
        for g in range(batch):
            tile = times_left(left_ref, half[g * BLOCK : (g + 1) * BLOCK]).astype(BF16)
            for k in range(LANES // 128):
                at = (first + g) * height + k * BLOCK
                block_ref[at : at + BLOCK, :] = tile[:, k * 128 : (k + 1) * 128]
        part = pl.ds(first * height, batch * height)
        for peer in range(out_ref.shape[0]):
            pltpu.make_async_copy(block_ref.at[part], out_ref.at[peer, part], sent).start()
    height = block_ref.shape[0]
    total = jnp.sum(jnp.sum(energy, axis=0, keepdims=True), axis=1, keepdims=True)
    at = iota(stamp_ref.shape, 0, jnp.int32)
    stamp = jnp.zeros(stamp_ref.shape, F32)
    for k in range(3):
        piece = total.astype(BF16).astype(F32)
        stamp = jnp.where(at == k, piece, stamp)
        total = total - piece
    stamp_ref[...] = stamp.astype(BF16)
    for peer in range(out_ref.shape[0]):
        pltpu.make_async_copy(stamp_ref, out_ref.at[peer, pl.ds(height, 8)], sent).start()
    pltpu.make_async_copy(out_ref, out_ref, sent).wait()


def combine(received, right, left, peers):
    sources, double, count = received.shape
    height = double // 2 * BLOCK
    block = (height * LANES // 128, 128)
    return pl.pallas_call(
        combine_kernel,
        in_specs=[VMEM] * 3,
        out_specs=HBM,
        out_shape=pltpu.HBM((peers, block[0] + 8, block[1]), BF16),
        scratch_shapes=[
            pltpu.VMEM((sources * double, count), F32),
            pltpu.VMEM((3 * double // 2, 128, 128), F32),
            pltpu.VMEM((height, LANES), F32),
            pltpu.VMEM(block, BF16),
            pltpu.VMEM((8, 128), BF16),
            pltpu.SemaphoreType.DMA,
        ],
        compiler_params=LIMIT,
        name="combine",
    )(received, right, left)


def total_kernel(in_ref, after_ref, out_ref):
    total = jnp.zeros((1, 1), F32)
    for share in range(in_ref.shape[0]):
        total = total + jnp.sum(in_ref[share, in_ref.shape[1] - 8 :, :].astype(F32)[:, :1], axis=0, keepdims=True)
    tile = out_ref.shape[1:]
    tile = jnp.where(iota(tile, 1, jnp.int32) == 0, total, 0.0)
    for peer in range(out_ref.shape[0]):
        out_ref[peer] = tile


def row_total(gathered, after, rows):
    return pl.pallas_call(
        total_kernel,
        in_specs=[VMEM, HBM],
        out_specs=VMEM,
        out_shape=pltpu.VMEM((rows, 1, 128), F32),
        compiler_params=LIMIT,
        name="row_total",
    )(gathered, after)


def scale_kernel(count, in_ref, energy_ref, out_ref, scaled_ref, stored):
    shares, height, lanes = in_ref.shape
    height = height - 8
    total = jnp.sum(energy_ref[...], axis=0)
    total = jnp.sum(jnp.sum(total, axis=0, keepdims=True), axis=1, keepdims=True)
    factor = lax.rsqrt(total * (1.0 / count) + EPSILON)
    stores = []
    pieces = height // BLOCK
    batch = shares * pieces // stored.shape[0]
    for piece in range(shares * pieces):
        inside = piece % pieces * BLOCK
        tile = in_ref[piece // pieces, inside : inside + BLOCK, :].astype(F32)
        scaled_ref[:, piece * lanes : (piece + 1) * lanes] = (tile * factor).astype(BF16)
        if (piece + 1) % batch == 0:
            part = (slice(None), pl.ds((piece + 1 - batch) * lanes, batch * lanes))
            stores.append(pltpu.make_async_copy(scaled_ref.at[part], out_ref.at[part], stored.at[piece // batch]))
            stores[-1].start()
    for store in stores:
        store.wait()


def scale(gathered, energies, count):
    shares, height, lanes = gathered.shape
    shape = (BLOCK, shares * (height - 8) // BLOCK * lanes)
    return pl.pallas_call(
        functools.partial(scale_kernel, count),
        in_specs=[VMEM, VMEM],
        out_specs=HBM,
        out_shape=pltpu.HBM(shape, BF16),
        scratch_shapes=[pltpu.VMEM(shape, BF16), pltpu.SemaphoreType.DMA((4,))],
        compiler_params=LIMIT,
        name="scale",
    )(gathered, energies)


def places():
    sizes = [lax.axis_size(axis) for axis in EVERY]
    return np.arange(np.prod(sizes)).reshape(sizes)


def share_holders(shares):
    place = places()
    groups = []
    for chip in range(place.shape[2]):
        groups.extend(place[:, :, chip, 0].T.reshape(-1, shares).tolist())
        groups.extend(place[:, :, chip, 1].reshape(-1, shares).tolist())
    return groups


def exchange(copies, groups):
    return lax.all_to_all(copies, EVERY, split_axis=0, concat_axis=0, axis_index_groups=groups, tiled=True)


def in_vmem(x):
    return pltpu.with_memory_space_constraint(x, pltpu.VMEM)


def in_hbm(x):
    return pltpu.with_memory_space_constraint(x, pltpu.HBM)


def local(gradient, momentum, indices):
    gradient, momentum = in_hbm(gradient[0]), in_hbm(momentum[0])
    height, columns = gradient.shape
    cosines = dct_basis()
    right, left = from_right(cosines.T), from_left(cosines)
    back_right, back_left = from_right(cosines), from_left(cosines.T)
    index = indices.reshape(indices.shape[-2:]).T
    rows = lax.axis_size(TENSOR)
    outgoing, index_rows = pick(gradient, momentum, in_hbm(index), in_hbm(right), in_hbm(left), SHARES)
    received = lax.all_to_all(outgoing, DP, split_axis=0, concat_axis=0, tiled=True)
    shared = combine(in_vmem(received), in_vmem(back_right), in_vmem(back_left), SHARES)
    new_momentum = remain(gradient, momentum, index_rows, right, left, back_right, back_left)
    gathered = in_vmem(exchange(shared, share_holders(SHARES)))
    energy = row_total(gathered, in_hbm(new_momentum), rows)
    energies = lax.all_to_all(energy, TENSOR, split_axis=0, concat_axis=0, tiled=True)
    update = scale(gathered, in_vmem(energies), height * columns * rows)
    return (new_momentum[None], update)


def solution(mesh):
    split = Mesh(mesh.devices.reshape(8, 8, 4, 2), ("dp_0", "dp_1", "tensor_0", "tensor_1"))
    placed = (P(DP, TENSOR, None), P(DP, TENSOR, None), P(DP, TENSOR, None, None))
    return jax.shard_map(
        local,
        mesh=split,
        in_specs=placed,
        out_specs=(P(DP, TENSOR, None), P(TENSOR, None)),
        check_vma=False,
    )
```

```python
import functools

import jax
import jax.numpy as jnp
import numpy as np
from jax import lax
from jax.experimental import pallas as pl
from jax.experimental.pallas import tpu as pltpu
from jax.sharding import Mesh
from jax.sharding import PartitionSpec as P

BLOCK = 64
LANES = 256
QUAD = 4
SHARES = 8
TENSOR = ("tensor_0", "tensor_1")
DP = ("dp_0", "dp_1")
EVERY = DP + TENSOR

EPSILON = 1e-06
DECAY = 0.999
F32 = jnp.float32
BF16 = jnp.bfloat16


def dct_basis():
    frequency = np.arange(BLOCK, dtype=np.float64)[:, None]
    position = np.arange(BLOCK, dtype=np.float64)[None, :]
    waves = np.cos(np.pi * (2.0 * position + 1.0) * frequency / (2.0 * BLOCK))
    return (waves * np.where(frequency == 0.0, np.sqrt(1.0 / BLOCK), np.sqrt(2.0 / BLOCK))).astype(np.float32)


def constant_halves(x):
    high = x.astype(BF16)
    return high, (x - high.astype(np.float32)).astype(BF16)


def from_left(cosines):
    high, low = constant_halves(cosines)
    return jnp.asarray(np.concatenate([high, high, low], axis=1))


def from_right(cosines):
    high, low = constant_halves(np.kron(np.eye(QUAD // 2, dtype=np.float32), cosines))
    return jnp.asarray(np.block([[high, low], [high, np.zeros_like(high)]]))


def halves(x):
    high = x.astype(BF16)
    return high, (x - high.astype(F32)).astype(BF16)


def dot(a, b):
    return lax.dot_general(a, b, (((1,), (0,)), ((), ())), preferred_element_type=F32)


def dot_t(a, b):
    return lax.dot_general(a, b, (((1,), (1,)), ((), ())), preferred_element_type=F32)


def times_right(tiles, right_ref):
    wide = LANES // 2
    cuts = [tiles[:, k * wide : (k + 1) * wide] for k in range(2)]
    both = jnp.concatenate([jnp.concatenate(halves(cut), axis=1) for cut in cuts], axis=0)
    product = dot(both, right_ref[...])
    product = product[:, :wide] + product[:, wide:]
    height = tiles.shape[0]
    return jnp.concatenate([product[:height], product[height:]], axis=1)


def times_left(left_ref, tile):
    high, low = halves(tile)
    return dot(left_ref[...], jnp.concatenate([high, low, high], axis=0))


def iota(shape, dim, kind=F32):
    return lax.broadcasted_iota(jnp.int32, shape, dim).astype(kind)


def hot(hit):
    return jnp.where(hit, jnp.ones(hit.shape, BF16), jnp.zeros(hit.shape, BF16))


def one_hot(hit):
    return jnp.where(hit, 1.0, 0.0).astype(BF16)


def col_hits(rows_ref, group, groups):
    col = rows_ref[pl.ds(groups + group, 1), :].astype(BF16)
    return hot(iota((LANES, col.shape[1]), 0).astype(BF16) == col)


def row_levels(rows_ref, group):
    row = rows_ref[pl.ds(group, 1), :]
    return row, iota((BLOCK, row.shape[1]), 0)


def spectra(gradient_ref, momentum_ref, right_ref, left_ref, tiles, first=0):
    cuts = [slice((first + t) * LANES, (first + t + 1) * LANES) for t in range(tiles)]
    renewed = [DECAY * momentum_ref[:, c].astype(F32) + gradient_ref[:, c].astype(F32) for c in cuts]
    half = times_right(jnp.concatenate(renewed, axis=0), right_ref)
    return renewed, [times_left(left_ref, half[t * BLOCK : (t + 1) * BLOCK]) for t in range(tiles)]


def lay_rows(index, rows_ref):
    selected, spans = index.shape
    groups, count = spans // QUAD, selected * QUAD
    copies = one_hot(iota((selected, count), 0, jnp.int32) == iota((selected, count), 1, jnp.int32) % selected)
    keep = iota((spans, count), 0, jnp.int32) % QUAD == iota((spans, count), 1, jnp.int32) // selected
    collect = one_hot(iota((groups, spans), 0, jnp.int32) == iota((groups, spans), 1, jnp.int32) // QUAD)
    span_start = (iota((1, count), 1, jnp.int32) // selected * BLOCK).astype(F32)
    for part, table in enumerate((index // BLOCK, index % BLOCK)):
        turned = jnp.transpose(table.astype(F32)).astype(BF16)
        laid = dot(collect, jnp.where(keep, dot(turned, copies), 0.0).astype(BF16))
        rows_ref[part * groups : (part + 1) * groups, :] = laid + span_start if part else laid


def pick_kernel(
    steps, gradient_in, momentum_in, index_in, right_in, left_in, out_ref, rows_ref,
    gradient_ref, momentum_ref, index_ref, right_ref, left_ref, payload_ref, loaded
):
    starts = np.cumsum([0, *steps])
    tables = [
        pltpu.make_async_copy(source, target, loaded.at[2 * len(steps) + k])
        for k, (source, target) in enumerate(((index_in, index_ref), (right_in, right_ref), (left_in, left_ref)))
    ]
    loads = []
    for step, tiles in enumerate(steps):
        part = (slice(None), pl.ds(int(starts[step]) * LANES, tiles * LANES))
        loads.append(
            [
                pltpu.make_async_copy(source.at[part], target.at[part], loaded.at[2 * step + k])
                for k, (source, target) in enumerate(((gradient_in, gradient_ref), (momentum_in, momentum_ref)))
            ]
        )
    for group in [tables, *loads]:
        for load in group:
            load.start()
    tables[0].wait()
    index = index_ref[...]
    groups = index.shape[1] // QUAD
    lay_rows(index, rows_ref)
    rows = []
    for load in tables[1:]:
        load.wait()
    for step, tiles in enumerate(steps):
        for load in loads[step]:
            load.wait()
        first = int(starts[step])
        _, spectrum = spectra(gradient_ref, momentum_ref, right_ref, left_ref, tiles, first)
        for t in range(tiles):
            by_col = dot(spectrum[t].astype(BF16), col_hits(rows_ref, first + t, groups))
            row, levels = row_levels(rows_ref, first + t)
            rows.append(jnp.sum(jnp.where(levels == row, by_col, 0.0), axis=0, keepdims=True))
    row = rows_ref[:groups, :].astype(jnp.int32)
    scale = jnp.ones(row.shape, F32)
    for bit in range(6):
        scale = jnp.where((row >> bit) & 1 == 1, scale * float(2 ** (2**bit)), scale)
    col = rows_ref[groups:, :].astype(jnp.int32) % BLOCK
    coded = (BLOCK + col).astype(F32) * scale
    picked = jnp.concatenate(rows, axis=0)
    shares = payload_ref.shape[0]
    own = groups // shares
    for share in range(shares):
        part = slice(share * own, (share + 1) * own)
        payload_ref[share] = jnp.concatenate([picked[part], coded[part]], axis=0).astype(BF16)
    core = lax.axis_index(TENSOR[1])
    line = lax.axis_size(DP[1])
    for peer in range(out_ref.shape[0]):
        along_first, along_second = peer // line % shares, peer % line % shares
        out_ref[peer] = payload_ref[along_first + (along_second - along_first) * core]


VMEM = pl.BlockSpec(memory_space=pltpu.VMEM)
HBM = pl.BlockSpec(memory_space=pltpu.HBM)
LIMIT = pltpu.CompilerParams(vmem_limit_bytes=24 * 2**20)


def whole(shape):
    return pl.BlockSpec(shape, lambda i: (0,) * len(shape))


def pick(gradient, momentum, index, right, left, shares, steps=(8, 24)):
    selected, spans = index.shape
    groups, count = spans // QUAD, selected * QUAD
    share_shape = (2 * groups // shares, count)
    return pl.pallas_call(
        functools.partial(pick_kernel, steps),
        in_specs=[HBM] * 5,
        out_specs=[VMEM, VMEM],
        out_shape=[pltpu.VMEM((lax.axis_size(DP), *share_shape), BF16), pltpu.VMEM((2 * groups, count), F32)],
        scratch_shapes=[
            pltpu.VMEM(gradient.shape, BF16),
            pltpu.VMEM(momentum.shape, BF16),
            pltpu.VMEM(index.shape, jnp.int32),
            pltpu.VMEM(right.shape, BF16),
            pltpu.VMEM(left.shape, BF16),
            pltpu.VMEM((shares, *share_shape), BF16),
            pltpu.SemaphoreType.DMA((2 * len(steps) + 3,)),
        ],
        name="pick",
    )(gradient, momentum, index, right, left)


def remain_kernel(tiles, gradient_ref, momentum_ref, rows_ref, right_ref, left_ref, back_right_ref, back_left_ref, out_ref):
    step = pl.program_id(0)
    groups = rows_ref.shape[0] // 2
    renewed, spectrum = spectra(gradient_ref, momentum_ref, right_ref, left_ref, tiles)
    kept = []
    for t in range(tiles):
        row, levels = row_levels(rows_ref, step * tiles + t)
        marker = dot_t(hot(levels.astype(BF16) == row.astype(BF16)), col_hits(rows_ref, step * tiles + t, groups))
        kept.append(spectrum[t] * marker)
    half = times_right(jnp.concatenate(kept, axis=0), back_right_ref)
    for t in range(tiles):
        restored = times_left(back_left_ref, half[t * BLOCK : (t + 1) * BLOCK])
        out_ref[:, t * LANES : (t + 1) * LANES] = (renewed[t] - restored).astype(BF16)


def remain(gradient, momentum, rows, right, left, back_right, back_left, steps=4):
    height, columns = gradient.shape
    width = columns // steps
    slab = pl.BlockSpec((height, width), lambda i: (0, i))
    return pl.pallas_call(
        functools.partial(remain_kernel, width // LANES),
        grid=(steps,),
        in_specs=[slab, slab, VMEM] + [whole(a.shape) for a in (right, left, back_right, back_left)],
        out_specs=slab,
        out_shape=jax.ShapeDtypeStruct((height, columns), BF16),
        name="remain",
        cost_estimate=pl.CostEstimate(flops=5_000_000_000, bytes_accessed=6 * height * columns, transcendentals=0),
    )(gradient, momentum, rows, right, left, back_right, back_left)


def combine_kernel(in_ref, right_ref, left_ref, out_ref, stage_ref, table_ref, sum_ref, block_ref, stamp_ref, sent):
    sources, double, count = in_ref.shape
    groups, selected = double // 2, count // QUAD
    halved = 128 // sources
    rows = selected // halved
    for source in range(sources):
        stage_ref[source * double : (source + 1) * double, :] = in_ref[source].astype(F32)

    def turned(table):
        shifted = [table] + [pltpu.roll(table, count - h * rows, 1) for h in range(1, halved)]
        return jnp.transpose(jnp.concatenate(shifted, axis=0))

    for g in range(groups):
        value = stage_ref[pl.ds(g, sources, stride=double), :]
        code = stage_ref[pl.ds(groups + g, sources, stride=double), :]
        row = jnp.zeros(code.shape, F32)
        for shift in (32, 16, 8, 4, 2, 1):
            above = code >= BLOCK * 2.0**shift
            code = jnp.where(above, code * 2.0**-shift, code)
            row = jnp.where(above, row + float(shift), row)
        for k, table in enumerate((value, row, code - float(BLOCK))):
            table_ref[3 * g + k] = turned(table)
    levels = iota((BLOCK, 2 * 128), 0).astype(BF16)
    zero = jnp.zeros(levels.shape, BF16)
    one = jnp.ones(levels.shape, BF16)
    energy = jnp.zeros((8, BLOCK), F32)
    for g in range(groups):
        parts = []
        for q in range(QUAD):
            total = None
            for r in range(0, rows, 2):
                at = q * selected + r
                value, row, col = (
                    jnp.concatenate([table_ref[3 * g + k, at + i : at + i + 1, :] for i in range(2)], axis=1).astype(BF16)
                    for k in range(3)
                )
                by_row = jnp.where(levels == row, jnp.broadcast_to(value, levels.shape), zero)
                term = dot_t(by_row, jnp.where(levels == col, one, zero))
                total = term if total is None else total + term
            square = total * total
            for r in range(0, BLOCK, 8):
                energy = energy + square[r : r + 8]
            parts.append(total)
        sum_ref[g * BLOCK : (g + 1) * BLOCK, :] = jnp.concatenate(parts, axis=1)
    height = BLOCK * (LANES // 128)
    batch = groups // 2
    for first in range(0, groups, batch):
        half = times_right(sum_ref[first * BLOCK : (first + batch) * BLOCK, :], right_ref)
        for g in range(batch):
            tile = times_left(left_ref, half[g * BLOCK : (g + 1) * BLOCK]).astype(BF16)
            for k in range(LANES // 128):
                at = (first + g) * height + k * BLOCK
                block_ref[at : at + BLOCK, :] = tile[:, k * 128 : (k + 1) * 128]
        part = pl.ds(first * height, batch * height)
        for peer in range(out_ref.shape[0]):
            pltpu.make_async_copy(block_ref.at[part], out_ref.at[peer, part], sent).start()
    height = block_ref.shape[0]
    total = jnp.sum(jnp.sum(energy, axis=0, keepdims=True), axis=1, keepdims=True)
    at = iota(stamp_ref.shape, 0, jnp.int32)
    stamp = jnp.zeros(stamp_ref.shape, F32)
    for k in range(3):
        piece = total.astype(BF16).astype(F32)
        stamp = jnp.where(at == k, piece, stamp)
        total = total - piece
    stamp_ref[...] = stamp.astype(BF16)
    for peer in range(out_ref.shape[0]):
        pltpu.make_async_copy(stamp_ref, out_ref.at[peer, pl.ds(height, 8)], sent).start()
    pltpu.make_async_copy(out_ref, out_ref, sent).wait()


def combine(received, right, left, peers):
    sources, double, count = received.shape
    height = double // 2 * BLOCK
    block = (height * LANES // 128, 128)
    return pl.pallas_call(
        combine_kernel,
        in_specs=[VMEM] * 3,
        out_specs=HBM,
        out_shape=pltpu.HBM((peers, block[0] + 8, block[1]), BF16),
        scratch_shapes=[
            pltpu.VMEM((sources * double, count), F32),
            pltpu.VMEM((3 * double // 2, 128, 128), F32),
            pltpu.VMEM((height, LANES), F32),
            pltpu.VMEM(block, BF16),
            pltpu.VMEM((8, 128), BF16),
            pltpu.SemaphoreType.DMA,
        ],
        compiler_params=LIMIT,
        name="combine",
    )(received, right, left)


def total_kernel(in_ref, after_ref, out_ref):
    total = jnp.zeros((1, 1), F32)
    for share in range(in_ref.shape[0]):
        total = total + jnp.sum(in_ref[share, in_ref.shape[1] - 8 :, :].astype(F32)[:, :1], axis=0, keepdims=True)
    tile = out_ref.shape[1:]
    tile = jnp.where(iota(tile, 1, jnp.int32) == 0, total, 0.0)
    for peer in range(out_ref.shape[0]):
        out_ref[peer] = tile


def row_total(gathered, after, rows):
    return pl.pallas_call(
        total_kernel,
        in_specs=[VMEM, HBM],
        out_specs=VMEM,
        out_shape=pltpu.VMEM((rows, 1, 128), F32),
        compiler_params=LIMIT,
        name="row_total",
    )(gathered, after)


def scale_kernel(count, in_ref, energy_ref, out_ref, scaled_ref, stored):
    shares, height, lanes = in_ref.shape
    height = height - 8
    total = jnp.sum(energy_ref[...], axis=0)
    total = jnp.sum(jnp.sum(total, axis=0, keepdims=True), axis=1, keepdims=True)
    factor = lax.rsqrt(total * (1.0 / count) + EPSILON)
    stores = []
    pieces = height // BLOCK
    batch = shares * pieces // stored.shape[0]
    for piece in range(shares * pieces):
        inside = piece % pieces * BLOCK
        tile = in_ref[piece // pieces, inside : inside + BLOCK, :].astype(F32)
        scaled_ref[:, piece * lanes : (piece + 1) * lanes] = (tile * factor).astype(BF16)
        if (piece + 1) % batch == 0:
            part = (slice(None), pl.ds((piece + 1 - batch) * lanes, batch * lanes))
            stores.append(pltpu.make_async_copy(scaled_ref.at[part], out_ref.at[part], stored.at[piece // batch]))
            stores[-1].start()
    for store in stores:
        store.wait()


def scale(gathered, energies, count):
    shares, height, lanes = gathered.shape
    shape = (BLOCK, shares * (height - 8) // BLOCK * lanes)
    return pl.pallas_call(
        functools.partial(scale_kernel, count),
        in_specs=[VMEM, VMEM],
        out_specs=HBM,
        out_shape=pltpu.HBM(shape, BF16),
        scratch_shapes=[pltpu.VMEM(shape, BF16), pltpu.SemaphoreType.DMA((4,))],
        compiler_params=LIMIT,
        name="scale",
    )(gathered, energies)


def places():
    sizes = [lax.axis_size(axis) for axis in EVERY]
    return np.arange(np.prod(sizes)).reshape(sizes)


def share_holders(shares):
    place = places()
    groups = []
    for chip in range(place.shape[2]):
        groups.extend(place[:, :, chip, 0].T.reshape(-1, shares).tolist())
        groups.extend(place[:, :, chip, 1].reshape(-1, shares).tolist())
    return groups


def exchange(copies, groups):
    return lax.all_to_all(copies, EVERY, split_axis=0, concat_axis=0, axis_index_groups=groups, tiled=True)


def in_vmem(x):
    return pltpu.with_memory_space_constraint(x, pltpu.VMEM)


def in_hbm(x):
    return pltpu.with_memory_space_constraint(x, pltpu.HBM)


def local(gradient, momentum, indices):
    gradient, momentum = in_hbm(gradient[0]), in_hbm(momentum[0])
    height, columns = gradient.shape
    cosines = dct_basis()
    right, left = from_right(cosines.T), from_left(cosines)
    back_right, back_left = from_right(cosines), from_left(cosines.T)
    index = indices.reshape(indices.shape[-2:]).T
    rows = lax.axis_size(TENSOR)
    outgoing, index_rows = pick(gradient, momentum, in_hbm(index), in_hbm(right), in_hbm(left), SHARES)
    received = lax.all_to_all(outgoing, DP, split_axis=0, concat_axis=0, tiled=True)
    shared = combine(in_vmem(received), in_vmem(back_right), in_vmem(back_left), SHARES)
    new_momentum = remain(gradient, momentum, index_rows, right, left, back_right, back_left)
    gathered = in_vmem(exchange(shared, share_holders(SHARES)))
    energy = row_total(gathered, in_hbm(new_momentum), rows)
    energies = lax.all_to_all(energy, TENSOR, split_axis=0, concat_axis=0, tiled=True)
    update = scale(gathered, in_vmem(energies), height * columns * rows)
    return (new_momentum[None], update)


def solution(mesh):
    split = Mesh(mesh.devices.reshape(8, 8, 4, 2), ("dp_0", "dp_1", "tensor_0", "tensor_1"))
    placed = (P(DP, TENSOR, None), P(DP, TENSOR, None), P(DP, TENSOR, None, None))
    return jax.shard_map(
        local,
        mesh=split,
        in_specs=placed,
        out_specs=(P(DP, TENSOR, None), P(TENSOR, None)),
        check_vma=False,
    )
```
